512 devices in a mesh: zero: 8 (over z), tp: 8 (over x, core), shift: 8 (over y).
Axes of the slice: x: 4, y: 8, z: 8, core: 2. Of those that a mesh axis runs over, the one named last changes fastest.
Arguments:
- train_gate: bfloat16 [16384, 8192], P(('shift', 'zero'), 'tp'), parts along dimension 0, may hold values from -0.125 to 0.125
- low_gate: bfloat16 [16384, 32], P(('shift', 'zero')), parts along dimension 0, may hold values from -0.125 to 0.125
- high_gate: bfloat16 [256, 8192], P('shift', 'tp'), parts along dimension 0, may hold values from -1 to 1
- train_up: bfloat16 [16384, 8192], P(('shift', 'zero'), 'tp'), parts along dimension 0, may hold values from -0.125 to 0.125
- low_up: bfloat16 [16384, 32], P(('shift', 'zero')), parts along dimension 0, may hold values from -0.125 to 0.125
- high_up: bfloat16 [256, 8192], P('shift', 'tp'), parts along dimension 0, may hold values from -1 to 1
- norm_train: float32 [16384], P(('shift', 'zero', 'tp')), parts along dimension 0, may hold values from 0.25 to 1.75
- norm_step: float32 [16384], P(('shift', 'zero', 'tp')), parts along dimension 0, may hold values from -0.3 to 0.3
Outputs:
- ready_gate: bfloat16 [65536, 2048], P(('shift', 'tp')), parts along dimension 0
- ready_up: bfloat16 [65536, 2048], P(('shift', 'tp')), parts along dimension 0
- serve_norm: bfloat16 [16384], P('shift'), parts along dimension 0
The draws below stay inside these ranges and needn't reach their ends.
There are 8 independent parts, one for each index of `shift`. The reference program is written for one: setup_inputs(seed, part) draws one part's arguments, and reference() takes and returns one part's arrays. A program takes and returns all parts, laid end to end along the dimension named above; each array names one. Nothing has to cross between parts.
All inputs are finite; a program needn't handle non-finite values.
Results may differ from the reference program's by a relative error of at most 0.001.
Values may be sent and summed in bfloat16 or wider, within the bound.
A program may use at most 64 MiB of HBM per device.

```python
import jax
import jax.numpy as jnp

D_MODEL = 2048
D_INNER = 8192
RANK = 32


def block_levels(own_key, dims, pieces, smallest, top_value):
    loudness = 1.0
    for position, parts in pieces:
        draws = jax.random.uniform(jax.random.fold_in(jax.random.fold_in(own_key, 6), position), (parts,), jnp.float32, smallest / len(pieces), top_value / len(pieces))
        loudness = loudness * jnp.repeat(jnp.exp(draws), dims[position] // parts).reshape((-1,) + (1,) * (len(dims) - 1 - position))
    return loudness


def scatter_about(rng, extent, spread, limit, pieces=(), kind=jnp.bfloat16):
    array = jax.random.normal(rng, extent, jnp.float32) * spread
    if len(pieces) > 0:
        array = block_levels(rng, extent, pieces, -0.22, 0.18) * array
    return jnp.clip(array, min=-limit, max=limit).astype(kind)


def setup_inputs(seed: int = 0, part: int = 0) -> dict:
    arg_keys = jax.random.split(jax.random.key(seed), 9)
    part_keys = jax.random.split(jax.random.fold_in(arg_keys[8], part), 9)
    return {
        "train_gate": scatter_about(part_keys[0], (D_MODEL, D_INNER), D_MODEL ** -0.5, 0.125, ((0, 8), (1, 8))),
        "low_gate": scatter_about(part_keys[1], (D_MODEL, RANK), D_MODEL ** -0.5, 0.125, ((0, 8),)),
        "high_gate": scatter_about(part_keys[2], (RANK, D_INNER), RANK ** -0.5, 1.0, ((1, 8),)),
        "train_up": scatter_about(part_keys[3], (D_MODEL, D_INNER), D_MODEL ** -0.5, 0.125, ((0, 8), (1, 8))),
        "low_up": scatter_about(part_keys[4], (D_MODEL, RANK), D_MODEL ** -0.5, 0.125, ((0, 8),)),
        "high_up": scatter_about(part_keys[5], (RANK, D_INNER), RANK ** -0.5, 1.0, ((1, 8),)),
        "norm_train": jnp.clip(1.0 + 0.15 * jax.random.normal(part_keys[6], (D_MODEL,), jnp.float32), 0.25, 1.75),
        "norm_step": jnp.clip(jax.random.uniform(part_keys[7], (D_MODEL,), jnp.float32, -0.3, 0.3) * block_levels(part_keys[7], (D_MODEL,), ((0, 64),), -0.4, 0.0), -0.3, 0.3),
    }


mix_rate = 0.5


def reference(train_gate, low_gate, high_gate, train_up, low_up, high_up, norm_train, norm_step):
    latest_gate = train_gate.astype(jnp.float32) + mix_rate * jnp.dot(low_gate, high_gate, preferred_element_type=jnp.float32)
    latest_up = train_up.astype(jnp.float32) + mix_rate * jnp.dot(low_up, high_up, preferred_element_type=jnp.float32)
    ready_gate = latest_gate.T.astype(jnp.bfloat16)
    ready_up = latest_up.T.astype(jnp.bfloat16)
    serve_norm = (norm_train + norm_step).astype(jnp.bfloat16)
    return ready_gate, ready_up, serve_norm
```

```python
import functools

import jax
import jax.numpy as jnp
from jax import lax
from jax.experimental import pallas as pl
from jax.experimental.pallas import tpu as pltpu
from jax.sharding import PartitionSpec as P

mix_rate = 0.5
MESH = pl.DeviceIdType.MESH
F32 = jnp.float32
BF16 = jnp.bfloat16
PIECES = 4


def ring_kernel(
    nz, nt,
    train_g, low_g, high_g, train_u, low_u, high_u, norm_a, norm_b,
    out_g, out_u, out_n,
    tg, tu, lg, lu, hg, hu, n_own, n_tp, n_zero, n_ring,
    in_sem, send_sem, recv_sem, tp_send, tp_recv, n_send, n_recv,
):
    z = lax.axis_index("zero")
    t = lax.axis_index("tp")
    right, left = lax.rem(z + 1, nz), lax.rem(z + nz - 1, nz)
    toward = (right, left)
    depth, width = tg.shape
    rows = width // PIECES
    far = nz // 2

    barrier = pltpu.get_barrier_semaphore()
    for peer in toward:
        pl.semaphore_signal(barrier, inc=1, device_id={"zero": peer}, device_id_type=MESH)
    for d in range(1, nt):
        pl.semaphore_signal(
            barrier, inc=1, device_id={"tp": lax.rem(t + d, nt)}, device_id_type=MESH
        )

    loads = []
    for k, (src, dst) in enumerate(((low_g, lg), (high_g, hg), (low_u, lu), (high_u, hu))):
        loads.append(pltpu.make_async_copy(src, dst, in_sem.at[k]))
    pieces = []
    for c in range(PIECES):
        cols = pl.ds(c * rows, rows)
        for p, (src, dst) in enumerate(((train_g, tg), (train_u, tu))):
            pieces.append(
                pltpu.make_async_copy(
                    src.at[:, cols], dst.at[:, cols], in_sem.at[4 + 2 * c + p]
                )
            )
    loads[0].start()
    loads[1].start()
    pieces[0].start()
    loads[2].start()
    loads[3].start()
    for copy in pieces[1:]:
        copy.start()

    both = norm_a[...] + norm_b[...]
    share = both.shape[1]
    per_row = 128 // share
    spot = z * nt + t
    line = jnp.concatenate([both] * per_row, axis=1)
    shape = n_own.shape
    row_id = lax.broadcasted_iota(jnp.int32, shape, 0)
    lane_id = lax.broadcasted_iota(jnp.int32, shape, 1)
    place = (row_id * 128 + lane_id) // share
    n_own[...] = jnp.where(place == spot, jnp.broadcast_to(line, shape), 0.0)

    outs = (out_g, out_u)
    trains, lows, highs = (tg, tu), (lg, lu), (hg, hu)

    def where(origin, i):
        c, p = divmod(i, 2)
        first = pl.multiple_of(origin * depth, depth)
        return outs[p].at[pl.ds(c * rows, rows), pl.ds(first, depth)]

    def compute(i):
        c, p = divmod(i, 2)
        cols = pl.ds(c * rows, rows)
        mixed = lax.dot_general(
            highs[p][:, cols], lows[p][...], (((0,), (0,)), ((), ())),
            preferred_element_type=F32,
        )
        base = trains[p][:, cols].T.astype(F32)
        where(z, i)[...] = (base + mix_rate * mixed).astype(BF16)

    def send(way, hop, i):
        origin = lax.rem(z + nz - hop, nz) if way == 0 else lax.rem(z + hop, nz)
        block = where(origin, i)
        return pltpu.make_async_remote_copy(
            src_ref=block, dst_ref=block,
            send_sem=send_sem.at[way, hop, i], recv_sem=recv_sem.at[way, hop, i],
            device_id={"zero": toward[way]}, device_id_type=MESH,
        )

    def landing(way, hop, i):
        origin = lax.rem(z + nz - hop - 1, nz) if way == 0 else lax.rem(z + hop + 1, nz)
        block = where(origin, i)
        return pltpu.make_async_remote_copy(
            src_ref=block, dst_ref=block,
            send_sem=send_sem.at[way, hop, i], recv_sem=recv_sem.at[way, hop, i],
            device_id={"zero": toward[way]}, device_id_type=MESH,
        )

    sent = []
    total = 2 * PIECES
    for i in range(total):
        if i < 2:
            loads[2 * i].wait()
            loads[2 * i + 1].wait()
        pieces[i].wait()
        compute(i)
        if i == 0:
            pl.semaphore_wait(barrier, 2 + nt - 1)
        for way in range(2):
            copy = send(way, 0, i)
            copy.start()
            sent.append(copy)

    tp_copies = []
    for d in range(1, nt):
        copy = pltpu.make_async_remote_copy(
            src_ref=n_own, dst_ref=n_tp.at[d],
            send_sem=tp_send.at[d], recv_sem=tp_recv.at[d],
            device_id={"tp": lax.rem(t + d, nt)}, device_id_type=MESH,
        )
        copy.start()
        tp_copies.append(copy)

    def norm_copy(way, hop):
        return pltpu.make_async_remote_copy(
            src_ref=n_zero if hop == 0 else n_ring.at[way, hop - 1],
            dst_ref=n_ring.at[way, hop],
            send_sem=n_send.at[way, hop], recv_sem=n_recv.at[way, hop],
            device_id={"zero": toward[way]}, device_id_type=MESH,
        )

    norm_hops = (far, nz - 1 - far)
    norm_sent = []

    def norm_step(hop):
        if hop == 0:
            acc = n_own[...]
            for copy in tp_copies:
                copy.wait()
            for d in range(1, nt):
                acc = acc + n_tp[d]
            n_zero[...] = acc
        for way in range(2):
            if hop > 0 and hop <= norm_hops[way]:
                norm_sent[2 * (hop - 1) + way].wait_recv()
        for way in range(2):
            if hop < norm_hops[way]:
                copy = norm_copy(way, hop)
                copy.start()
                norm_sent.append(copy)

    def last_hop(way, i):
        return far - 1 if i % 2 == way else nz - 2 - far

    for hop in range(1, far + 1):
        for i in range(total):
            for way in range(2):
                if hop - 1 <= last_hop(way, i):
                    landing(way, hop - 1, i).wait_recv()
                    if hop <= last_hop(way, i):
                        copy = send(way, hop, i)
                        copy.start()
                        sent.append(copy)
        if hop == 1:
            norm_step(0)
        if hop == 2:
            norm_step(1)
            norm_step(2)
            norm_step(3)
            norm_step(4)
            acc = n_zero[...]
            for way in range(2):
                for h in range(norm_hops[way]):
                    acc = acc + n_ring[way, h]
            out_n[...] = acc.astype(BF16)

    for copy in sent:
        copy.wait_send()
    for copy in norm_sent:
        copy.wait_send()


def body(train_gate, low_gate, high_gate, train_up, low_up, high_up, norm_train, norm_step):
    nz, nt = lax.axis_size("zero"), lax.axis_size("tp")
    depth, width = train_gate.shape
    rank = low_gate.shape[1]
    share = norm_train.shape[0]
    whole = nz * depth
    tile = (whole // 128, 128)
    far = nz // 2
    hbm = pl.BlockSpec(memory_space=pltpu.HBM)
    vmem = pl.BlockSpec(memory_space=pltpu.VMEM)
    dma = pltpu.SemaphoreType.DMA
    gate, up, norm = pl.pallas_call(
        functools.partial(ring_kernel, nz, nt),
        out_shape=(
            pltpu.VMEM((width, whole), BF16),
            pltpu.VMEM((width, whole), BF16),
            pltpu.VMEM(tile, BF16),
        ),
        in_specs=[hbm] * 6 + [vmem] * 2,
        out_specs=(vmem,) * 3,
        scratch_shapes=[
            pltpu.VMEM((depth, width), BF16),
            pltpu.VMEM((depth, width), BF16),
            pltpu.VMEM((rank, depth), BF16),
            pltpu.VMEM((rank, depth), BF16),
            pltpu.VMEM((rank, width), BF16),
            pltpu.VMEM((rank, width), BF16),
            pltpu.VMEM(tile, F32),
            pltpu.VMEM((nt, *tile), F32),
            pltpu.VMEM(tile, F32),
            pltpu.VMEM((2, far, *tile), F32),
            dma((4 + 2 * PIECES,)),
            dma((2, far, 2 * PIECES)),
            dma((2, far, 2 * PIECES)),
            dma((nt,)),
            dma((nt,)),
            dma((2, far)),
            dma((2, far)),
        ],
        compiler_params=pltpu.CompilerParams(
            collective_id=0, has_side_effects=True, vmem_limit_bytes=24 * 1024 * 1024
        ),
    )(
        train_gate, low_gate.T, high_gate, train_up, low_up.T, high_up,
        norm_train.reshape(1, share), norm_step.reshape(1, share),
    )
    return gate, up, norm.reshape(whole)


def solution(mesh):
    in_specs = (
        P(("shift", "zero"), "tp"),
        P(("shift", "zero"), None),
        P("shift", "tp"),
        P(("shift", "zero"), "tp"),
        P(("shift", "zero"), None),
        P("shift", "tp"),
        P(("shift", "zero", "tp")),
        P(("shift", "zero", "tp")),
    )
    out_specs = (P(("shift", "tp"), None), P(("shift", "tp"), None), P("shift"))
    return jax.shard_map(body, mesh=mesh, in_specs=in_specs, out_specs=out_specs, check_vma=False)
```

```python
import functools

import jax
import jax.numpy as jnp
from jax import lax
from jax.experimental import pallas as pl
from jax.experimental.pallas import tpu as pltpu
from jax.sharding import PartitionSpec as P

mix_rate = 0.5
MESH = pl.DeviceIdType.MESH
F32 = jnp.float32
BF16 = jnp.bfloat16
GATE, UP = 0, 1
RIGHT, LEFT = 0, 1

OWN = ((GATE, 0, 1), (GATE, 1, 2), (GATE, 2, 4), (GATE, 4, 8), (UP, 0, 2), (UP, 2, 4), (UP, 4, 8))
OWN_BOTH = 4
PASSED = ((GATE, 0, 4), (GATE, 4, 8), (UP, 0, 4), (UP, 4, 8))
LAST = tuple((p, 2 * k, 2 * k + 2) for p in (GATE, UP) for k in range(4))
SLOTS = 8


def ring_kernel(
    nz, nt,
    train_g, low_g, high_g, train_u, low_u, high_u, norm_a, norm_b,
    out_g, out_u, out_n,
    tg, tu, lg, lu, hg, hu, na, nb, n_own, n_tp, n_all,
    in_sem, send_sem, recv_sem, tp_send, tp_recv, n_send, n_recv, go,
):
    z = lax.axis_index("zero")
    t = lax.axis_index("tp")
    right, left = lax.rem(z + 1, nz), lax.rem(z + nz - 1, nz)
    toward = (right, left)
    depth, width = tg.shape
    eighth = width // 8
    hops = nz // 2
    end, sink = nz - 1, nz - 2

    barrier = pltpu.get_barrier_semaphore()

    @pl.when(z < sink)
    def _():
        pl.semaphore_signal(barrier, inc=1, device_id={"zero": right}, device_id_type=MESH)

    @pl.when((z == 0) | (z == end))
    def _():
        pl.semaphore_signal(barrier, inc=1, device_id={"zero": left}, device_id_type=MESH)

    for d in range(1, nt):
        pl.semaphore_signal(
            barrier, inc=1, device_id={"tp": lax.rem(t + d, nt)}, device_id_type=MESH
        )

    outs = (out_g, out_u)
    sources = ((train_g, low_g, high_g), (train_u, low_u, high_u))
    holds = ((tg, lg, hg), (tu, lu, hu))

    loads = {}
    for p in (GATE, UP):
        for k in (1, 2):
            loads[p, k] = pltpu.make_async_copy(
                sources[p][k], holds[p][k], in_sem.at[2 * p + k - 1]
            )
    pieces = []
    for i, (p, a, b) in enumerate(OWN):
        cols = pl.ds(a * eighth, (b - a) * eighth)
        pieces.append(
            pltpu.make_async_copy(
                sources[p][0].at[:, cols], holds[p][0].at[:, cols], in_sem.at[6 + i]
            )
        )
    norm_loads = (
        pltpu.make_async_copy(norm_a, na, in_sem.at[4]),
        pltpu.make_async_copy(norm_b, nb, in_sem.at[5]),
    )
    loads[GATE, 1].start()
    loads[GATE, 2].start()
    for i in range(OWN_BOTH):
        pieces[i].start()
    for copy in norm_loads:
        copy.start()
    loads[UP, 1].start()
    loads[UP, 2].start()
    for i in range(OWN_BOTH, len(OWN)):
        pieces[i].start()

    def where(origin, piece):
        p, a, b = piece
        first = pl.multiple_of(origin * depth, depth)
        return outs[p].at[pl.ds(a * eighth, (b - a) * eighth), pl.ds(first, depth)]

    def compute(piece):
        p, a, b = piece
        train, low, high = holds[p]
        cols = pl.ds(a * eighth, (b - a) * eighth)
        mixed = lax.dot_general(
            high[:, cols], low[...], (((0,), (0,)), ((), ())), preferred_element_type=F32
        )
        base = train[:, cols].T.astype(F32)
        where(z, piece)[...] = (base + mix_rate * mixed).astype(BF16)

    def copy_of(way, hop, i, piece, back):
        gone = hop + back
        origin = lax.rem(z + nz - gone, nz) if way == RIGHT else lax.rem(z + gone, nz)
        block = where(origin, piece)
        return pltpu.make_async_remote_copy(
            src_ref=block, dst_ref=block,
            send_sem=send_sem.at[way, hop, i], recv_sem=recv_sem.at[way, hop, i],
            device_id={"zero": toward[way]}, device_id_type=MESH,
        )

    def norm_copy(way, hop, back):
        gone = hop + back
        origin = lax.rem(z + nz - gone, nz) if way == RIGHT else lax.rem(z + gone, nz)
        return pltpu.make_async_remote_copy(
            src_ref=n_all.at[origin], dst_ref=n_all.at[origin],
            send_sem=n_send.at[way, hop], recv_sem=n_recv.at[way, hop],
            device_id={"zero": toward[way]}, device_id_type=MESH,
        )

    right_first = (z == 0) | (z == end)

    loads[GATE, 1].wait()
    loads[GATE, 2].wait()
    pieces[0].wait()
    compute(OWN[0])

    pl.semaphore_wait(
        barrier,
        nt - 1 + jnp.where(z == 0, 0, 1) + jnp.where(z == sink, 1, 0),
    )

    @pl.when((z > 0) & (z < end))
    def _():
        pl.semaphore_signal(go.at[LEFT], inc=1, device_id={"zero": left}, device_id_type=MESH)

    @pl.when(z >= sink)
    def _():
        pl.semaphore_signal(go.at[RIGHT], inc=1, device_id={"zero": right}, device_id_type=MESH)

    @pl.when(z == 0)
    def _():
        pl.semaphore_wait(go.at[LEFT], 1)

    def first_way(i):
        @pl.when(right_first)
        def _():
            copy_of(RIGHT, 0, i, OWN[i], 0).start()

        @pl.when(jnp.logical_not(right_first))
        def _():
            copy_of(LEFT, 0, i, OWN[i], 0).start()

    def second_way(i):
        @pl.when(right_first)
        def _():
            copy_of(LEFT, 0, i, OWN[i], 0).start()

        @pl.when(jnp.logical_not(right_first))
        def _():
            copy_of(RIGHT, 0, i, OWN[i], 0).start()

    first_way(0)
    for i in range(1, OWN_BOTH):
        pieces[i].wait()
        compute(OWN[i])
        first_way(i)

    @pl.when((z > 0) & (z < sink))
    def _():
        pl.semaphore_wait(go.at[LEFT], 1)

    @pl.when((z == 0) | (z == end))
    def _():
        pl.semaphore_wait(go.at[RIGHT], 1)

    for i in range(OWN_BOTH):
        second_way(i)

    for copy in norm_loads:
        copy.wait()
    both = na[...] + nb[...]
    share = both.shape[1]
    line = jnp.concatenate([both] * (128 // share), axis=1)
    shape = n_own.shape
    place = (
        lax.broadcasted_iota(jnp.int32, shape, 0) * 128
        + lax.broadcasted_iota(jnp.int32, shape, 1)
    )
    mine = (place >= t * share) & (place < (t + 1) * share)
    n_own[...] = jnp.where(mine, jnp.broadcast_to(line, shape), 0.0)

    loads[UP, 1].wait()
    loads[UP, 2].wait()
    tp_copies = []
    for i in range(OWN_BOTH, len(OWN)):
        pieces[i].wait()
        compute(OWN[i])
        first_way(i)
        second_way(i)
        if i == OWN_BOTH:
            for d in range(1, nt):
                copy = pltpu.make_async_remote_copy(
                    src_ref=n_own, dst_ref=n_tp.at[d],
                    send_sem=tp_send.at[d], recv_sem=tp_recv.at[d],
                    device_id={"tp": lax.rem(t + d, nt)}, device_id_type=MESH,
                )
                copy.start()
                tp_copies.append(copy)

    acc = n_own[...]
    for copy in tp_copies:
        copy.wait()
    for d in range(1, nt):
        acc = acc + n_tp[d]
    n_all[z] = acc

    norm_hops = (hops, nz - 1 - hops)
    norm_sent = [(way, 0) for way in (RIGHT, LEFT)]
    for way, hop in norm_sent:
        norm_copy(way, hop, 0).start()

    def norm_on(hop):
        for way in (RIGHT, LEFT):
            if hop - 1 < norm_hops[way]:
                norm_copy(way, hop - 1, 1).wait_recv()
            if hop < norm_hops[way]:
                norm_copy(way, hop, 0).start()
                norm_sent.append((way, hop))

    def pieces_of(hop):
        return OWN if hop == 0 else LAST if hop == hops - 1 else PASSED

    def guarded(way, hop, i, dest, act):
        if hop < hops - 1:
            act()
            return
        p, k = divmod(i, 4)
        if p == GATE and k == 3:
            pl.when(dest != 0 if way == RIGHT else dest == 0)(act)
        elif p == UP and k == 0:
            pl.when(dest == end if way == RIGHT else dest != end)(act)
        elif p == way:
            act()

    waited = set()

    def land(way, hop, piece):
        p, a, b = piece
        for i, (q, c, d) in enumerate(pieces_of(hop)):
            if q == p and c < b and d > a and (way, hop, i) not in waited:
                waited.add((way, hop, i))
                copy_of(way, hop, i, pieces_of(hop)[i], 1).wait_recv()

    for hop in range(1, hops):
        if hop > 1:
            norm_on(hop)
        for i, piece in enumerate(pieces_of(hop)):
            if hop == 1 and i == len(pieces_of(hop)) // 2:
                norm_on(hop)
            for way in (RIGHT, LEFT):
                land(way, hop - 1, piece)
                guarded(way, hop, i, toward[way], lambda: copy_of(way, hop, i, piece, 0).start())

    norm_on(hops)
    out_n[...] = jnp.concatenate([n_all[k] for k in range(nz)], axis=0).astype(BF16)

    for i, piece in enumerate(LAST):
        for way in (RIGHT, LEFT):
            guarded(way, hops - 1, i, z, lambda: copy_of(way, hops - 1, i, piece, 1).wait_recv())

    for hop in range(hops):
        for i, piece in enumerate(pieces_of(hop)):
            for way in (RIGHT, LEFT):
                guarded(way, hop, i, toward[way], lambda: copy_of(way, hop, i, piece, 0).wait_send())
    for way, hop in norm_sent:
        norm_copy(way, hop, 0).wait_send()


def store_kernel(gate, up, norm, out_g, out_u, out_n, sem):
    copies = []
    rows = gate.shape[0] // 4
    for k in range(4):
        part = pl.ds(k * rows, rows)
        copies.append(pltpu.make_async_copy(gate.at[part], out_g.at[part], sem.at[2 * k]))
        copies.append(pltpu.make_async_copy(up.at[part], out_u.at[part], sem.at[2 * k + 1]))
    copies.append(pltpu.make_async_copy(norm, out_n, sem.at[8]))
    for copy in copies:
        copy.start()
    for copy in copies:
        copy.wait()


def body(train_gate, low_gate, high_gate, train_up, low_up, high_up, norm_train, norm_step):
    nz, nt = lax.axis_size("zero"), lax.axis_size("tp")
    depth, width = train_gate.shape
    rank = low_gate.shape[1]
    share = norm_train.shape[0]
    whole = nz * depth
    lines = depth // 128
    hbm = pl.BlockSpec(memory_space=pltpu.HBM)
    vmem = pl.BlockSpec(memory_space=pltpu.VMEM)
    dma = pltpu.SemaphoreType.DMA
    inputs = (
        train_gate, low_gate.T, high_gate, train_up, low_up.T, high_up,
        norm_train.reshape(1, share), norm_step.reshape(1, share),
    )
    gate, up, norm = pl.pallas_call(
        functools.partial(ring_kernel, nz, nt),
        out_shape=(
            pltpu.VMEM((width, whole), BF16),
            pltpu.VMEM((width, whole), BF16),
            pltpu.VMEM((nz * lines, 128), BF16),
        ),
        in_specs=[hbm] * 8,
        out_specs=(vmem,) * 3,
        scratch_shapes=[
            pltpu.VMEM((depth, width), BF16),
            pltpu.VMEM((depth, width), BF16),
            pltpu.VMEM((rank, depth), BF16),
            pltpu.VMEM((rank, depth), BF16),
            pltpu.VMEM((rank, width), BF16),
            pltpu.VMEM((rank, width), BF16),
            pltpu.VMEM((1, share), F32),
            pltpu.VMEM((1, share), F32),
            pltpu.VMEM((lines, 128), F32),
            pltpu.VMEM((nt, lines, 128), F32),
            pltpu.VMEM((nz, lines, 128), F32),
            dma((6 + len(OWN),)),
            dma((2, nz // 2, SLOTS)),
            dma((2, nz // 2, SLOTS)),
            dma((nt,)),
            dma((nt,)),
            dma((2, nz // 2)),
            dma((2, nz // 2)),
            pltpu.SemaphoreType.REGULAR((2,)),
        ],
        compiler_params=pltpu.CompilerParams(
            collective_id=0, has_side_effects=True, vmem_limit_bytes=24 * 1024 * 1024
        ),
    )(*(pltpu.with_memory_space_constraint(x, pltpu.HBM) for x in inputs))
    gate, up, norm = pl.pallas_call(
        store_kernel,
        out_shape=(
            jax.ShapeDtypeStruct((width, whole), BF16),
            jax.ShapeDtypeStruct((width, whole), BF16),
            jax.ShapeDtypeStruct((nz * lines, 128), BF16),
        ),
        in_specs=[vmem] * 3,
        out_specs=(hbm,) * 3,
        scratch_shapes=[dma((9,))],
        compiler_params=pltpu.CompilerParams(vmem_limit_bytes=24 * 1024 * 1024),
    )(gate, up, norm)
    return gate, up, norm.reshape(whole)


def solution(mesh):
    in_specs = (
        P(("shift", "zero"), "tp"),
        P(("shift", "zero"), None),
        P("shift", "tp"),
        P(("shift", "zero"), "tp"),
        P(("shift", "zero"), None),
        P("shift", "tp"),
        P(("shift", "zero", "tp")),
        P(("shift", "zero", "tp")),
    )
    out_specs = (P(("shift", "tp"), None), P(("shift", "tp"), None), P("shift"))
    return jax.shard_map(body, mesh=mesh, in_specs=in_specs, out_specs=out_specs, check_vma=False)
```

```python
import functools

import jax
import jax.numpy as jnp
from jax import lax
from jax.experimental import pallas as pl
from jax.experimental.pallas import tpu as pltpu
from jax.sharding import PartitionSpec as P

mix_rate = 0.5
MESH = pl.DeviceIdType.MESH
F32 = jnp.float32
BF16 = jnp.bfloat16
GATE, UP = 0, 1
RIGHT, LEFT = 0, 1

OWN = ((GATE, 0, 1), (GATE, 1, 2), (GATE, 2, 4), (GATE, 4, 8), (UP, 0, 2), (UP, 2, 4), (UP, 4, 8))
OWN_BOTH = 4
PASSED = ((GATE, 0, 4), (GATE, 4, 8), (UP, 0, 4), (UP, 4, 8))
LAST = tuple((p, 2 * k, 2 * k + 2) for p in (GATE, UP) for k in range(4))
SLOTS = 8


def ring_kernel(
    nz, nt,
    train_g, low_g, high_g, train_u, low_u, high_u, norm_a, norm_b,
    out_g, out_u, out_n,
    tg, tu, lg, lu, hg, hu, na, nb, n_own, n_hub, n_tp,
    in_sem, send_sem, recv_sem, tp_send, tp_recv, hub_send, hub_recv, n_send, n_recv, go,
):
    z = lax.axis_index("zero")
    t = lax.axis_index("tp")
    right, left = lax.rem(z + 1, nz), lax.rem(z + nz - 1, nz)
    toward = (right, left)
    depth, width = tg.shape
    eighth = width // 8
    hops = nz // 2
    end, sink = nz - 1, nz - 2

    outs = (out_g, out_u)
    sources = ((train_g, low_g, high_g), (train_u, low_u, high_u))
    holds = ((tg, lg, hg), (tu, lu, hu))

    loads = {}
    for p in (GATE, UP):
        for k in (1, 2):
            loads[p, k] = pltpu.make_async_copy(
                sources[p][k], holds[p][k], in_sem.at[2 * p + k - 1]
            )
    pieces = []
    for i, (p, a, b) in enumerate(OWN):
        cols = pl.ds(a * eighth, (b - a) * eighth)
        pieces.append(
            pltpu.make_async_copy(
                sources[p][0].at[:, cols], holds[p][0].at[:, cols], in_sem.at[6 + i]
            )
        )
    norm_loads = (
        pltpu.make_async_copy(norm_a, na, in_sem.at[4]),
        pltpu.make_async_copy(norm_b, nb, in_sem.at[5]),
    )
    loads[GATE, 1].start()
    loads[GATE, 2].start()
    pieces[0].start()

    barrier = pltpu.get_barrier_semaphore()

    @pl.when(z == 0)
    def _():
        for k in range(1, nz):
            pl.semaphore_signal(barrier, inc=1, device_id={"zero": k}, device_id_type=MESH)
        for d in range(1, nt):
            pl.semaphore_signal(
                barrier, inc=1, device_id={"tp": lax.rem(t + d, nt)}, device_id_type=MESH
            )

    @pl.when((z > 0) & (z < sink))
    def _():
        pl.semaphore_signal(barrier, inc=1, device_id={"zero": right}, device_id_type=MESH)

    @pl.when(z == end)
    def _():
        pl.semaphore_signal(barrier, inc=1, device_id={"zero": left}, device_id_type=MESH)

    @pl.when(z > 0)
    def _():
        pl.semaphore_wait(
            barrier,
            1 + jnp.where((z > 1) & (z < end), 1, 0) + jnp.where(z == sink, 1, 0),
        )

    @pl.when((z > 0) & (z < end))
    def _():
        pl.semaphore_signal(go.at[LEFT], inc=1, device_id={"zero": left}, device_id_type=MESH)

    @pl.when(z >= sink)
    def _():
        pl.semaphore_signal(go.at[RIGHT], inc=1, device_id={"zero": right}, device_id_type=MESH)

    for i in range(1, OWN_BOTH):
        pieces[i].start()
    for copy in norm_loads:
        copy.start()

    def where(origin, piece):
        p, a, b = piece
        first = pl.multiple_of(origin * depth, depth)
        return outs[p].at[pl.ds(a * eighth, (b - a) * eighth), pl.ds(first, depth)]

    def compute(piece):
        p, a, b = piece
        train, low, high = holds[p]
        cols = pl.ds(a * eighth, (b - a) * eighth)
        mixed = lax.dot_general(
            high[:, cols], low[...], (((0,), (0,)), ((), ())), preferred_element_type=F32
        )
        base = train[:, cols].T.astype(F32)
        where(z, piece)[...] = (base + mix_rate * mixed).astype(BF16)

    def copy_of(way, hop, i, piece, back):
        gone = hop + back
        origin = lax.rem(z + nz - gone, nz) if way == RIGHT else lax.rem(z + gone, nz)
        block = where(origin, piece)
        return pltpu.make_async_remote_copy(
            src_ref=block, dst_ref=block,
            send_sem=send_sem.at[way, hop, i], recv_sem=recv_sem.at[way, hop, i],
            device_id={"zero": toward[way]}, device_id_type=MESH,
        )

    right_first = (z == 0) | (z == end)

    def first_way(i):
        @pl.when(right_first)
        def _():
            copy_of(RIGHT, 0, i, OWN[i], 0).start()

        @pl.when(jnp.logical_not(right_first))
        def _():
            copy_of(LEFT, 0, i, OWN[i], 0).start()

    def second_way(i):
        @pl.when(right_first)
        def _():
            copy_of(LEFT, 0, i, OWN[i], 0).start()

        @pl.when(jnp.logical_not(right_first))
        def _():
            copy_of(RIGHT, 0, i, OWN[i], 0).start()

    loads[GATE, 1].wait()
    loads[GATE, 2].wait()
    pieces[0].wait()
    compute(OWN[0])

    @pl.when(z == 0)
    def _():
        pl.semaphore_wait(go.at[LEFT], 1)

    first_way(0)
    loads[UP, 1].start()
    loads[UP, 2].start()
    for i in range(OWN_BOTH, len(OWN)):
        pieces[i].start()
    pieces[1].wait()
    compute(OWN[1])
    first_way(1)

    for copy in norm_loads:
        copy.wait()
    both = na[...] + nb[...]
    share = both.shape[1]
    line = jnp.concatenate([both] * (128 // share), axis=1)
    shape = n_own.shape
    spot = (
        lax.broadcasted_iota(jnp.int32, shape, 0) * 128
        + lax.broadcasted_iota(jnp.int32, shape, 1)
    )
    mine = (spot >= t * share) & (spot < (t + 1) * share)
    n_own[...] = jnp.where(mine, jnp.broadcast_to(line, shape), 0.0)
    to_hub = pltpu.make_async_remote_copy(
        src_ref=n_own, dst_ref=n_hub.at[z], send_sem=hub_send, recv_sem=hub_recv.at[z],
        device_id={"zero": 0}, device_id_type=MESH,
    )

    for i in range(2, OWN_BOTH):
        pieces[i].wait()
        compute(OWN[i])
        first_way(i)
        if i == 2:
            pl.when(z > 0)(to_hub.start)

    @pl.when((z > 0) & (z < sink))
    def _():
        pl.semaphore_wait(go.at[LEFT], 1)

    @pl.when((z == 0) | (z == end))
    def _():
        pl.semaphore_wait(go.at[RIGHT], 1)

    for i in range(OWN_BOTH):
        second_way(i)

    loads[UP, 1].wait()
    loads[UP, 2].wait()
    for i in range(OWN_BOTH, len(OWN)):
        pieces[i].wait()
        compute(OWN[i])
        first_way(i)
        second_way(i)

    def to_all(k):
        return pltpu.make_async_remote_copy(
            src_ref=out_n, dst_ref=out_n, send_sem=n_send.at[k], recv_sem=n_recv,
            device_id={"zero": k}, device_id_type=MESH,
        )

    @pl.when(z == 0)
    def _():
        n_hub[0] = n_own[...]
        pl.semaphore_wait(barrier, nt - 1)
        for k in range(1, nz):
            pltpu.make_async_remote_copy(
                src_ref=n_own, dst_ref=n_hub.at[k], send_sem=hub_send, recv_sem=hub_recv.at[k],
                device_id={"zero": end}, device_id_type=MESH,
            ).wait_recv()
        copies = []
        for d in range(1, nt):
            copy = pltpu.make_async_remote_copy(
                src_ref=n_hub, dst_ref=n_tp.at[d],
                send_sem=tp_send.at[d], recv_sem=tp_recv.at[d],
                device_id={"tp": lax.rem(t + d, nt)}, device_id_type=MESH,
            )
            copy.start()
            copies.append(copy)
        acc = n_hub[...]
        for d in range(1, nt):
            copies[d - 1].wait()
            acc = acc + n_tp[d]
        out_n[...] = jnp.concatenate([acc[k] for k in range(nz)], axis=0).astype(BF16)
        for k in range(1, nz):
            to_all(k).start()

    def pieces_of(hop):
        return OWN if hop == 0 else LAST if hop == hops - 1 else PASSED

    def guarded(way, hop, i, dest, act):
        if hop < hops - 1:
            act()
            return
        p, k = divmod(i, 4)
        if p == GATE and k == 3:
            pl.when(dest != 0 if way == RIGHT else dest == 0)(act)
        elif p == UP and k == 0:
            pl.when(dest == end if way == RIGHT else dest != end)(act)
        elif p == way:
            act()

    waited = set()

    def land(way, hop, piece):
        p, a, b = piece
        for i, (q, c, d) in enumerate(pieces_of(hop)):
            if q == p and c < b and d > a and (way, hop, i) not in waited:
                waited.add((way, hop, i))
                copy_of(way, hop, i, pieces_of(hop)[i], 1).wait_recv()

    for hop in range(1, hops):
        for i, piece in enumerate(pieces_of(hop)):
            for way in (RIGHT, LEFT):
                land(way, hop - 1, piece)
                guarded(way, hop, i, toward[way], lambda: copy_of(way, hop, i, piece, 0).start())

    for i, piece in enumerate(LAST):
        for way in (RIGHT, LEFT):
            guarded(way, hops - 1, i, z, lambda: copy_of(way, hops - 1, i, piece, 1).wait_recv())

    for hop in range(hops):
        for i, piece in enumerate(pieces_of(hop)):
            for way in (RIGHT, LEFT):
                guarded(way, hop, i, toward[way], lambda: copy_of(way, hop, i, piece, 0).wait_send())

    @pl.when(z == 0)
    def _():
        for k in range(1, nz):
            to_all(k).wait_send()

    @pl.when(z > 0)
    def _():
        to_hub.wait_send()
        to_all(0).wait_recv()


def store_kernel(gate, up, norm, out_g, out_u, out_n, sem):
    copies = []
    rows = gate.shape[0] // 4
    for k in range(4):
        part = pl.ds(k * rows, rows)
        copies.append(pltpu.make_async_copy(gate.at[part], out_g.at[part], sem.at[2 * k]))
        copies.append(pltpu.make_async_copy(up.at[part], out_u.at[part], sem.at[2 * k + 1]))
    copies.append(pltpu.make_async_copy(norm, out_n, sem.at[8]))
    for copy in copies:
        copy.start()
    for copy in copies:
        copy.wait()


def body(train_gate, low_gate, high_gate, train_up, low_up, high_up, norm_train, norm_step):
    nz, nt = lax.axis_size("zero"), lax.axis_size("tp")
    depth, width = train_gate.shape
    rank = low_gate.shape[1]
    share = norm_train.shape[0]
    whole = nz * depth
    lines = depth // 128
    hbm = pl.BlockSpec(memory_space=pltpu.HBM)
    vmem = pl.BlockSpec(memory_space=pltpu.VMEM)
    dma = pltpu.SemaphoreType.DMA
    inputs = (
        train_gate, low_gate.T, high_gate, train_up, low_up.T, high_up,
        norm_train.reshape(1, share), norm_step.reshape(1, share),
    )
    gate, up, norm = pl.pallas_call(
        functools.partial(ring_kernel, nz, nt),
        out_shape=(
            pltpu.VMEM((width, whole), BF16),
            pltpu.VMEM((width, whole), BF16),
            pltpu.VMEM((nz * lines, 128), BF16),
        ),
        in_specs=[hbm] * 8,
        out_specs=(vmem,) * 3,
        scratch_shapes=[
            pltpu.VMEM((depth, width), BF16),
            pltpu.VMEM((depth, width), BF16),
            pltpu.VMEM((rank, depth), BF16),
            pltpu.VMEM((rank, depth), BF16),
            pltpu.VMEM((rank, width), BF16),
            pltpu.VMEM((rank, width), BF16),
            pltpu.VMEM((1, share), F32),
            pltpu.VMEM((1, share), F32),
            pltpu.VMEM((lines, 128), F32),
            pltpu.VMEM((nz, lines, 128), F32),
            pltpu.VMEM((nt, nz, lines, 128), F32),
            dma((6 + len(OWN),)),
            dma((2, nz // 2, SLOTS)),
            dma((2, nz // 2, SLOTS)),
            dma((nt,)),
            dma((nt,)),
            dma(()),
            dma((nz,)),
            dma((nz,)),
            dma(()),
            pltpu.SemaphoreType.REGULAR((2,)),
        ],
        compiler_params=pltpu.CompilerParams(
            collective_id=0, has_side_effects=True, vmem_limit_bytes=24 * 1024 * 1024
        ),
    )(*(pltpu.with_memory_space_constraint(x, pltpu.HBM) for x in inputs))
    gate, up, norm = pl.pallas_call(
        store_kernel,
        out_shape=(
            jax.ShapeDtypeStruct((width, whole), BF16),
            jax.ShapeDtypeStruct((width, whole), BF16),
            jax.ShapeDtypeStruct((nz * lines, 128), BF16),
        ),
        in_specs=[vmem] * 3,
        out_specs=(hbm,) * 3,
        scratch_shapes=[dma((9,))],
        compiler_params=pltpu.CompilerParams(vmem_limit_bytes=24 * 1024 * 1024),
    )(gate, up, norm)
    return gate, up, norm.reshape(whole)


def solution(mesh):
    in_specs = (
        P(("shift", "zero"), "tp"),
        P(("shift", "zero"), None),
        P("shift", "tp"),
        P(("shift", "zero"), "tp"),
        P(("shift", "zero"), None),
        P("shift", "tp"),
        P(("shift", "zero", "tp")),
        P(("shift", "zero", "tp")),
    )
    out_specs = (P(("shift", "tp"), None), P(("shift", "tp"), None), P("shift"))
    return jax.shard_map(body, mesh=mesh, in_specs=in_specs, out_specs=out_specs, check_vma=False)
```

```python
import functools

import jax
import jax.numpy as jnp
from jax import lax
from jax.experimental import pallas as pl
from jax.experimental.pallas import tpu as pltpu
from jax.sharding import PartitionSpec as P

mix_rate = 0.5
MESH = pl.DeviceIdType.MESH
F32 = jnp.float32
BF16 = jnp.bfloat16
GATE, UP = 0, 1
RIGHT, LEFT = 0, 1

OWN = ((GATE, 0, 2), (GATE, 2, 8), (GATE, 8, 16), (UP, 0, 8), (UP, 8, 16))
OWN_GATE = 3
PASSED = (
    ((GATE, 0, 8), (GATE, 8, 16), (UP, 0, 8), (UP, 8, 16)),
    ((UP, 0, 8), (UP, 8, 16), (GATE, 0, 8), (GATE, 8, 16)),
)
SWAP_GATE, SWAP_UP = (GATE, 11, 16), (UP, 0, 2)
SLOTS = 5


def ring_kernel(
    nz, nt,
    train_g, low_g, high_g, train_u, low_u, high_u, norm_a, norm_b,
    out_g, out_u, out_n,
    tg, tu, lg, lu, hg, hu, na, nb, n_own, n_hub, n_tp,
    in_sem, send_sem, recv_sem, tp_send, tp_recv, hub_send, hub_recv, n_send, n_recv, go,
):
    z = lax.axis_index("zero")
    t = lax.axis_index("tp")
    right, left = lax.rem(z + 1, nz), lax.rem(z + nz - 1, nz)
    toward = (right, left)
    depth, width = tg.shape
    part = width // 16
    hops = nz // 2
    end, sink = nz - 1, nz - 2

    outs = (out_g, out_u)
    sources = ((train_g, low_g, high_g), (train_u, low_u, high_u))
    holds = ((tg, lg, hg), (tu, lu, hu))

    loads = {}
    for p in (GATE, UP):
        for k in (1, 2):
            loads[p, k] = pltpu.make_async_copy(
                sources[p][k], holds[p][k], in_sem.at[k - 1]
            )
    trains = []
    for p, a, b, k in ((GATE, 0, 2, 2), (GATE, 2, 16, 3), (UP, 0, 16, 2)):
        cols = pl.ds(a * part, (b - a) * part)
        trains.append(
            pltpu.make_async_copy(sources[p][0].at[:, cols], holds[p][0].at[:, cols], in_sem.at[k])
        )
    norm_loads = (
        pltpu.make_async_copy(norm_a, na, in_sem.at[4]),
        pltpu.make_async_copy(norm_b, nb, in_sem.at[5]),
    )
    loads[GATE, 1].start()
    loads[GATE, 2].start()
    trains[0].start()

    barrier = pltpu.get_barrier_semaphore()

    @pl.when(z == 0)
    def _():
        for k in range(1, nz):
            pl.semaphore_signal(barrier, inc=1, device_id={"zero": k}, device_id_type=MESH)
        for d in range(1, nt):
            pl.semaphore_signal(
                barrier, inc=1, device_id={"tp": lax.rem(t + d, nt)}, device_id_type=MESH
            )

    @pl.when((z > 0) & (z < sink))
    def _():
        pl.semaphore_signal(barrier, inc=1, device_id={"zero": right}, device_id_type=MESH)

    @pl.when(z == end)
    def _():
        pl.semaphore_signal(barrier, inc=1, device_id={"zero": left}, device_id_type=MESH)

    @pl.when(z > 0)
    def _():
        pl.semaphore_wait(
            barrier,
            1 + jnp.where((z > 1) & (z < end), 1, 0) + jnp.where(z == sink, 1, 0),
        )

    @pl.when((z > 0) & (z < end))
    def _():
        pl.semaphore_signal(go.at[LEFT], inc=1, device_id={"zero": left}, device_id_type=MESH)

    @pl.when(z >= sink)
    def _():
        pl.semaphore_signal(go.at[RIGHT], inc=1, device_id={"zero": right}, device_id_type=MESH)

    trains[1].start()
    for copy in norm_loads:
        copy.start()

    def where(origin, piece):
        p, a, b = piece
        first = pl.multiple_of(origin * depth, depth)
        return outs[p].at[pl.ds(a * part, (b - a) * part), pl.ds(first, depth)]

    def compute(piece):
        p, a, b = piece
        train, low, high = holds[p]
        cols = pl.ds(a * part, (b - a) * part)
        mixed = lax.dot_general(
            high[:, cols], low[...], (((0,), (0,)), ((), ())), preferred_element_type=F32
        )
        base = train[:, cols].T.astype(F32)
        where(z, piece)[...] = (base + mix_rate * mixed).astype(BF16)

    def copy_of(way, hop, i, piece, back):
        gone = hop + back
        origin = lax.rem(z + nz - gone, nz) if way == RIGHT else lax.rem(z + gone, nz)
        block = where(origin, piece)
        return pltpu.make_async_remote_copy(
            src_ref=block, dst_ref=block,
            send_sem=send_sem.at[way, 0 if hop < hops - 1 else 1 + i],
            recv_sem=recv_sem.at[way, i if hop == 0 else SLOTS + 4 * (hop - 1) + i],
            device_id={"zero": toward[way]}, device_id_type=MESH,
        )

    right_first = (z == 0) | (z == end)

    def first_way(i):
        @pl.when(right_first)
        def _():
            copy_of(RIGHT, 0, i, OWN[i], 0).start()

        @pl.when(jnp.logical_not(right_first))
        def _():
            copy_of(LEFT, 0, i, OWN[i], 0).start()

    def second_way(i):
        @pl.when(right_first)
        def _():
            copy_of(LEFT, 0, i, OWN[i], 0).start()

        @pl.when(jnp.logical_not(right_first))
        def _():
            copy_of(RIGHT, 0, i, OWN[i], 0).start()

    loads[GATE, 1].wait()
    loads[GATE, 2].wait()
    trains[0].wait()
    compute(OWN[0])

    @pl.when(z == 0)
    def _():
        pl.semaphore_wait(go.at[LEFT], 1)

    first_way(0)
    loads[UP, 1].start()
    loads[UP, 2].start()
    trains[2].start()
    trains[1].wait()
    compute(OWN[1])
    first_way(1)

    for copy in norm_loads:
        copy.wait()
    both = na[...] + nb[...]
    share = both.shape[1]
    line = jnp.concatenate([both] * (128 // share), axis=1)
    shape = n_own.shape
    spot = (
        lax.broadcasted_iota(jnp.int32, shape, 0) * 128
        + lax.broadcasted_iota(jnp.int32, shape, 1)
    )
    mine = (spot >= t * share) & (spot < (t + 1) * share)
    n_own[...] = jnp.where(mine, jnp.broadcast_to(line, shape), 0.0)
    to_hub = pltpu.make_async_remote_copy(
        src_ref=n_own, dst_ref=n_hub.at[z], send_sem=hub_send, recv_sem=hub_recv,
        device_id={"zero": 0}, device_id_type=MESH,
    )

    pl.when(z > 0)(to_hub.start)
    for i in range(2, OWN_GATE):
        compute(OWN[i])
        first_way(i)

    @pl.when((z > 0) & (z < sink))
    def _():
        pl.semaphore_wait(go.at[LEFT], 1)

    @pl.when((z == 0) | (z == end))
    def _():
        pl.semaphore_wait(go.at[RIGHT], 1)

    for i in range(OWN_GATE):
        second_way(i)

    loads[UP, 1].wait()
    loads[UP, 2].wait()
    trains[2].wait()
    for i in range(OWN_GATE, len(OWN)):
        compute(OWN[i])
        first_way(i)
        second_way(i)

    def to_all(k):
        return pltpu.make_async_remote_copy(
            src_ref=out_n, dst_ref=out_n, send_sem=n_send, recv_sem=n_recv,
            device_id={"zero": k}, device_id_type=MESH,
        )

    @pl.when(z == 0)
    def _():
        n_hub[0] = n_own[...]
        pl.semaphore_wait(barrier, nt - 1)
        rest = n_hub.at[pl.ds(1, nz - 1)]
        pltpu.make_async_remote_copy(
            src_ref=rest, dst_ref=rest, send_sem=hub_send, recv_sem=hub_recv,
            device_id={"zero": end}, device_id_type=MESH,
        ).wait_recv()
        for d in range(1, nt):
            pltpu.make_async_remote_copy(
                src_ref=n_hub, dst_ref=n_tp.at[d], send_sem=tp_send, recv_sem=tp_recv,
                device_id={"tp": lax.rem(t + d, nt)}, device_id_type=MESH,
            ).start()
        rest = n_tp.at[pl.ds(1, nt - 1)]
        pltpu.make_async_remote_copy(
            src_ref=rest, dst_ref=rest, send_sem=tp_send, recv_sem=tp_recv,
            device_id={"tp": lax.rem(t + 1, nt)}, device_id_type=MESH,
        ).wait()
        acc = n_hub[...]
        for d in range(1, nt):
            acc = acc + n_tp[d]
        out_n[...] = jnp.concatenate([acc[k] for k in range(nz)], axis=0).astype(BF16)
        for k in range(1, nz):
            to_all(k).start()

    def pieces_of(way, hop):
        return OWN if hop == 0 else PASSED[way]

    def last_of(way, dest):
        if way == RIGHT:
            return (
                ((GATE, 0, SWAP_GATE[1]), None),
                (SWAP_GATE, dest != 0),
                (SWAP_UP, dest == end),
            )
        return (
            (SWAP_UP, dest != end),
            ((UP, SWAP_UP[2], 16), None),
            (SWAP_GATE, dest == 0),
        )

    def guarded(cond, act):
        if cond is None:
            act()
        else:
            pl.when(cond)(act)

    waited = set()

    def land(way, hop, piece):
        p, a, b = piece
        for i, (q, c, d) in enumerate(pieces_of(way, hop)):
            if q == p and c < b and d > a and (way, hop, i) not in waited:
                waited.add((way, hop, i))
                copy_of(way, hop, i, pieces_of(way, hop)[i], 1).wait_recv()

    for hop in range(1, hops - 1):
        for i in range(len(PASSED[RIGHT])):
            for way in (RIGHT, LEFT):
                piece = PASSED[way][i]
                land(way, hop - 1, piece)
                copy_of(way, hop, i, piece, 0).start()

    hop = hops - 1
    for i in range(3):
        for way in (RIGHT, LEFT):
            piece, cond = last_of(way, toward[way])[i]
            land(way, hop - 1, piece)
            guarded(cond, copy_of(way, hop, i, piece, 0).start)
    for way in (RIGHT, LEFT):
        for p in (GATE, UP):
            land(way, hop - 1, (p, 0, 16))

    for i in range(3):
        for way in (RIGHT, LEFT):
            piece, cond = last_of(way, z)[i]
            guarded(cond, copy_of(way, hop, i, piece, 1).wait_recv)

    for i in range(3):
        for way in (RIGHT, LEFT):
            piece, cond = last_of(way, toward[way])[i]
            guarded(cond, copy_of(way, hop, i, piece, 0).wait_send)
    for way in (RIGHT, LEFT):
        sent = out_g.at[pl.ds(0, (hops - 1) * 2 * depth * width // out_g.shape[1])]
        pltpu.make_async_remote_copy(
            src_ref=sent, dst_ref=sent, send_sem=send_sem.at[way, 0], recv_sem=recv_sem.at[way, 0],
            device_id={"zero": toward[way]}, device_id_type=MESH,
        ).wait_send()

    @pl.when(z == 0)
    def _():
        sent = out_g.at[pl.ds(0, (nz - 1) * out_n.shape[0]), pl.ds(0, out_n.shape[1])]
        pltpu.make_async_remote_copy(
            src_ref=sent, dst_ref=sent, send_sem=n_send, recv_sem=n_recv,
            device_id={"zero": end}, device_id_type=MESH,
        ).wait_send()

    @pl.when(z > 0)
    def _():
        to_hub.wait_send()
        to_all(0).wait_recv()


def store_kernel(gate, up, norm, out_g, out_u, out_n, sem):
    copies = []
    rows = gate.shape[0] // 4
    for k in range(4):
        part = pl.ds(k * rows, rows)
        copies.append(pltpu.make_async_copy(gate.at[part], out_g.at[part], sem.at[2 * k]))
        copies.append(pltpu.make_async_copy(up.at[part], out_u.at[part], sem.at[2 * k + 1]))
    copies.append(pltpu.make_async_copy(norm, out_n, sem.at[8]))
    for copy in copies:
        copy.start()
    for copy in copies:
        copy.wait()


def body(train_gate, low_gate, high_gate, train_up, low_up, high_up, norm_train, norm_step):
    nz, nt = lax.axis_size("zero"), lax.axis_size("tp")
    depth, width = train_gate.shape
    rank = low_gate.shape[1]
    share = norm_train.shape[0]
    whole = nz * depth
    lines = depth // 128
    hbm = pl.BlockSpec(memory_space=pltpu.HBM)
    vmem = pl.BlockSpec(memory_space=pltpu.VMEM)
    dma = pltpu.SemaphoreType.DMA
    inputs = (
        train_gate, low_gate.T, high_gate, train_up, low_up.T, high_up,
        norm_train.reshape(1, share), norm_step.reshape(1, share),
    )
    gate, up, norm = pl.pallas_call(
        functools.partial(ring_kernel, nz, nt),
        out_shape=(
            pltpu.VMEM((width, whole), BF16),
            pltpu.VMEM((width, whole), BF16),
            pltpu.VMEM((nz * lines, 128), BF16),
        ),
        in_specs=[hbm] * 8,
        out_specs=(vmem,) * 3,
        scratch_shapes=[
            pltpu.VMEM((depth, width), BF16),
            pltpu.VMEM((depth, width), BF16),
            pltpu.VMEM((rank, depth), BF16),
            pltpu.VMEM((rank, depth), BF16),
            pltpu.VMEM((rank, width), BF16),
            pltpu.VMEM((rank, width), BF16),
            pltpu.VMEM((1, share), F32),
            pltpu.VMEM((1, share), F32),
            pltpu.VMEM((lines, 128), F32),
            pltpu.VMEM((nz, lines, 128), F32),
            pltpu.VMEM((nt, nz, lines, 128), F32),
            dma((6,)),
            dma((2, 4)),
            dma((2, SLOTS + 2 * 4 + 3)),
            dma(()),
            dma(()),
            dma(()),
            dma(()),
            dma(()),
            dma(()),
            pltpu.SemaphoreType.REGULAR((2,)),
        ],
        compiler_params=pltpu.CompilerParams(
            collective_id=0, has_side_effects=True, vmem_limit_bytes=24 * 1024 * 1024
        ),
    )(*(pltpu.with_memory_space_constraint(x, pltpu.HBM) for x in inputs))
    gate, up, norm = pl.pallas_call(
        store_kernel,
        out_shape=(
            jax.ShapeDtypeStruct((width, whole), BF16),
            jax.ShapeDtypeStruct((width, whole), BF16),
            jax.ShapeDtypeStruct((nz * lines, 128), BF16),
        ),
        in_specs=[vmem] * 3,
        out_specs=(hbm,) * 3,
        scratch_shapes=[dma((9,))],
        compiler_params=pltpu.CompilerParams(vmem_limit_bytes=24 * 1024 * 1024),
    )(gate, up, norm)
    return gate, up, norm.reshape(whole)


def solution(mesh):
    in_specs = (
        P(("shift", "zero"), "tp"),
        P(("shift", "zero"), None),
        P("shift", "tp"),
        P(("shift", "zero"), "tp"),
        P(("shift", "zero"), None),
        P("shift", "tp"),
        P(("shift", "zero", "tp")),
        P(("shift", "zero", "tp")),
    )
    out_specs = (P(("shift", "tp"), None), P(("shift", "tp"), None), P("shift"))
    return jax.shard_map(body, mesh=mesh, in_specs=in_specs, out_specs=out_specs, check_vma=False)
```

```python
import functools

import jax
import jax.numpy as jnp
from jax import lax
from jax.experimental import pallas as pl
from jax.experimental.pallas import tpu as pltpu
from jax.sharding import PartitionSpec as P

mix_rate = 0.5
MESH = pl.DeviceIdType.MESH
F32 = jnp.float32
BF16 = jnp.bfloat16
GATE, UP = 0, 1
RIGHT, LEFT = 0, 1

OWN = ((GATE, 0, 2), (GATE, 2, 8), (GATE, 8, 16), (UP, 0, 8), (UP, 8, 16))
OWN_GATE = 3
G0, G1, U0, U1 = (GATE, 0, 8), (GATE, 8, 16), (UP, 0, 8), (UP, 8, 16)
PASSED = (None, ((G0, G1, U0, U1), (G0, U0, G1, U1)), ((G0, G1, U0, U1), (U0, G0, U1, G1)))
SWAP_GATE, SWAP_UP = (GATE, 11, 16), (UP, 0, 2)
SLOTS = len(OWN) + 2 * 4 + 1


def ring_kernel(
    nz, nt,
    train_g, low_g, high_g, train_u, low_u, high_u, norm_a, norm_b,
    out_g, out_u, out_n,
    tg, tu, lg, lu, hg, hu, na, nb, n_own, n_hub, n_tp,
    in_sem, send_sem, recv_sem, sent_sem, came_sem, tp_sem, go,
):
    z = lax.axis_index("zero")
    t = lax.axis_index("tp")
    right, left = lax.rem(z + 1, nz), lax.rem(z + nz - 1, nz)
    toward = (right, left)
    depth, width = tg.shape
    part = width // 16
    hops = nz // 2
    end, sink = nz - 1, nz - 2

    outs = (out_g, out_u)
    sources = ((train_g, low_g, high_g), (train_u, low_u, high_u))
    holds = ((tg, lg, hg), (tu, lu, hu))

    head, tail = pl.ds(0, 2 * part), pl.ds(2 * part, 14 * part)
    first_high = pltpu.make_async_copy(high_g.at[:, head], hg.at[:, head], in_sem.at[1])
    loads = {
        (GATE, 1): pltpu.make_async_copy(low_g, lg, in_sem.at[0]),
        (GATE, 2): pltpu.make_async_copy(high_g.at[:, tail], hg.at[:, tail], in_sem.at[6]),
        (UP, 1): pltpu.make_async_copy(low_u, lu, in_sem.at[0]),
        (UP, 2): pltpu.make_async_copy(high_u, hu, in_sem.at[1]),
    }
    trains = []
    for p, a, b, k in ((GATE, 0, 2, 2), (GATE, 2, 16, 3), (UP, 0, 16, 2)):
        cols = pl.ds(a * part, (b - a) * part)
        trains.append(
            pltpu.make_async_copy(sources[p][0].at[:, cols], holds[p][0].at[:, cols], in_sem.at[k])
        )
    norm_loads = (
        pltpu.make_async_copy(norm_a, na, in_sem.at[4]),
        pltpu.make_async_copy(norm_b, nb, in_sem.at[5]),
    )
    trains[0].start()
    loads[GATE, 1].start()
    first_high.start()

    barrier = pltpu.get_barrier_semaphore()

    @pl.when(z == 0)
    def _():
        for k in range(1, nz):
            pl.semaphore_signal(barrier, inc=1, device_id={"zero": k}, device_id_type=MESH)
        for d in range(1, nt):
            pl.semaphore_signal(
                barrier, inc=1, device_id={"tp": lax.rem(t + d, nt)}, device_id_type=MESH
            )

    @pl.when((z > 0) & (z < sink))
    def _():
        pl.semaphore_signal(barrier, inc=1, device_id={"zero": right}, device_id_type=MESH)

    @pl.when(z == end)
    def _():
        pl.semaphore_signal(barrier, inc=1, device_id={"zero": left}, device_id_type=MESH)

    @pl.when(z > 0)
    def _():
        pl.semaphore_wait(
            barrier,
            1 + jnp.where((z > 1) & (z < end), 1, 0) + jnp.where(z == sink, 1, 0),
        )

    @pl.when((z > 0) & (z < end))
    def _():
        pl.semaphore_signal(go.at[LEFT], inc=1, device_id={"zero": left}, device_id_type=MESH)

    @pl.when(z >= sink)
    def _():
        pl.semaphore_signal(go.at[RIGHT], inc=1, device_id={"zero": right}, device_id_type=MESH)

    loads[GATE, 2].start()
    trains[1].start()
    for copy in norm_loads:
        copy.start()

    def where(origin, piece):
        p, a, b = piece
        first = pl.multiple_of(origin * depth, depth)
        return outs[p].at[pl.ds(a * part, (b - a) * part), pl.ds(first, depth)]

    def compute(piece):
        p, a, b = piece
        train, low, high = holds[p]
        cols = pl.ds(a * part, (b - a) * part)
        mixed = lax.dot_general(
            high[:, cols], low[...], (((0,), (0,)), ((), ())), preferred_element_type=F32
        )
        base = train[:, cols].T.astype(F32)
        where(z, piece)[...] = (base + mix_rate * mixed).astype(BF16)

    def slot(hop, i):
        return i if hop == 0 else SLOTS - 1 if hop == hops - 1 else len(OWN) + 4 * (hop - 1) + i

    def copy_of(way, hop, i, piece, back):
        gone = hop + back
        origin = lax.rem(z + nz - gone, nz) if way == RIGHT else lax.rem(z + gone, nz)
        block = where(origin, piece)
        return pltpu.make_async_remote_copy(
            src_ref=block, dst_ref=block,
            send_sem=send_sem.at[way],
            recv_sem=recv_sem.at[way, slot(hop, i)],
            device_id={"zero": toward[way]}, device_id_type=MESH,
        )

    right_first = (z == 0) | (z == end)

    def first_way(i):
        @pl.when(right_first)
        def _():
            copy_of(RIGHT, 0, i, OWN[i], 0).start()

        @pl.when(jnp.logical_not(right_first))
        def _():
            copy_of(LEFT, 0, i, OWN[i], 0).start()

    def second_way(i):
        @pl.when(right_first)
        def _():
            copy_of(LEFT, 0, i, OWN[i], 0).start()

        @pl.when(jnp.logical_not(right_first))
        def _():
            copy_of(RIGHT, 0, i, OWN[i], 0).start()

    loads[GATE, 1].wait()
    first_high.wait()
    trains[0].wait()
    compute(OWN[0])

    @pl.when(z == 0)
    def _():
        pl.semaphore_wait(go.at[LEFT], 1)

    first_way(0)
    loads[UP, 1].start()
    loads[UP, 2].start()
    trains[2].start()
    loads[GATE, 2].wait()
    trains[1].wait()
    compute(OWN[1])
    first_way(1)

    for copy in norm_loads:
        copy.wait()
    both = na[...] + nb[...]
    share = both.shape[1]
    line = jnp.concatenate([both] * (128 // share), axis=1)
    shape = n_own.shape
    spot = (
        lax.broadcasted_iota(jnp.int32, shape, 0) * 128
        + lax.broadcasted_iota(jnp.int32, shape, 1)
    )
    mine = (spot >= t * share) & (spot < (t + 1) * share)
    n_own[...] = jnp.where(mine, jnp.broadcast_to(line, shape), 0.0)
    to_hub = pltpu.make_async_remote_copy(
        src_ref=n_own, dst_ref=n_hub.at[z], send_sem=sent_sem, recv_sem=came_sem,
        device_id={"zero": 0}, device_id_type=MESH,
    )

    pl.when(z > 0)(to_hub.start)
    for i in range(2, OWN_GATE):
        compute(OWN[i])
        first_way(i)

    @pl.when((z > 0) & (z < sink))
    def _():
        pl.semaphore_wait(go.at[LEFT], 1)

    @pl.when((z == 0) | (z == end))
    def _():
        pl.semaphore_wait(go.at[RIGHT], 1)

    for i in range(OWN_GATE):
        second_way(i)

    loads[UP, 1].wait()
    loads[UP, 2].wait()
    trains[2].wait()
    for i in range(OWN_GATE, len(OWN)):
        compute(OWN[i])
        first_way(i)
        second_way(i)

    def to_all(k):
        return pltpu.make_async_remote_copy(
            src_ref=out_n, dst_ref=out_n, send_sem=sent_sem, recv_sem=came_sem,
            device_id={"zero": k}, device_id_type=MESH,
        )

    @pl.when(z == 0)
    def _():
        n_hub[0] = n_own[...]
        pl.semaphore_wait(barrier, nt - 1)
        rest = n_hub.at[pl.ds(1, nz - 1)]
        pltpu.make_async_remote_copy(
            src_ref=rest, dst_ref=rest, send_sem=sent_sem, recv_sem=came_sem,
            device_id={"zero": end}, device_id_type=MESH,
        ).wait_recv()
        for d in range(1, nt):
            pltpu.make_async_remote_copy(
                src_ref=n_hub, dst_ref=n_tp.at[d], send_sem=sent_sem, recv_sem=tp_sem,
                device_id={"tp": lax.rem(t + d, nt)}, device_id_type=MESH,
            ).start()
        rest = n_tp.at[pl.ds(1, nt - 1)]
        pltpu.make_async_remote_copy(
            src_ref=rest, dst_ref=rest, send_sem=sent_sem, recv_sem=tp_sem,
            device_id={"tp": lax.rem(t + 1, nt)}, device_id_type=MESH,
        ).wait()
        acc = n_hub[...]
        for d in range(1, nt):
            acc = acc + n_tp[d]
        out_n[...] = jnp.concatenate([acc[k] for k in range(nz)], axis=0).astype(BF16)
        for k in range(1, nz):
            to_all(k).start()

    def pieces_of(way, hop):
        return OWN if hop == 0 else PASSED[hop][way]

    def last_of(way, dest):
        if way == RIGHT:
            return (
                ((GATE, 0, SWAP_GATE[1]), None),
                (SWAP_GATE, dest != 0),
                (SWAP_UP, dest == end),
            )
        return (
            (SWAP_UP, dest != end),
            ((UP, SWAP_UP[2], 16), None),
            (SWAP_GATE, dest == 0),
        )

    def guarded(cond, act):
        if cond is None:
            act()
        else:
            pl.when(cond)(act)

    waited = set()

    def land(way, hop, piece):
        p, a, b = piece
        for i, (q, c, d) in enumerate(pieces_of(way, hop)):
            if q == p and c < b and d > a and (way, hop, i) not in waited:
                waited.add((way, hop, i))
                copy_of(way, hop, i, pieces_of(way, hop)[i], 1).wait_recv()

    for hop in range(1, hops - 1):
        for i in range(4):
            for way in (RIGHT, LEFT):
                piece = PASSED[hop][way][i]
                land(way, hop - 1, piece)
                copy_of(way, hop, i, piece, 0).start()

    hop = hops - 1
    for i in range(3):
        for way in (RIGHT, LEFT):
            piece, cond = last_of(way, toward[way])[i]
            land(way, hop - 1, piece)
            guarded(cond, copy_of(way, hop, i, piece, 0).start)
    for way in (RIGHT, LEFT):
        for p in (GATE, UP):
            land(way, hop - 1, (p, 0, 16))

    swap_gate, swap_up = (p[2] - p[1] for p in (SWAP_GATE, SWAP_UP))

    def total(way, dest, before, act):
        rows = part * depth // out_g.shape[1]
        base = before + 16 * rows
        more, less = (swap_up, swap_gate) if way == RIGHT else (swap_gate, swap_up)
        gains, loses = (end, 0) if way == RIGHT else (0, end)
        for cond, count in (
            (dest == gains, base + more * rows),
            (dest == loses, base - less * rows),
            ((dest != gains) & (dest != loses), base),
        ):
            block = out_g.at[pl.ds(0, count)]
            copy = pltpu.make_async_remote_copy(
                src_ref=block, dst_ref=block,
                send_sem=send_sem.at[way], recv_sem=recv_sem.at[way, SLOTS - 1],
                device_id={"zero": toward[way]}, device_id_type=MESH,
            )
            pl.when(cond)(functools.partial(act, copy))

    for way in (LEFT, RIGHT):
        total(way, z, 0, lambda copy: copy.wait_recv())
    for way in (RIGHT, LEFT):
        total(way, toward[way], (hops - 1) * 2 * depth * width // out_g.shape[1], lambda copy: copy.wait_send())

    @pl.when(z == 0)
    def _():
        sent = out_g.at[pl.ds(0, (nz - 1) * out_n.shape[0]), pl.ds(0, out_n.shape[1])]
        pltpu.make_async_remote_copy(
            src_ref=sent, dst_ref=sent, send_sem=sent_sem, recv_sem=came_sem,
            device_id={"zero": end}, device_id_type=MESH,
        ).wait_send()

    @pl.when(z > 0)
    def _():
        to_hub.wait_send()
        to_all(0).wait_recv()


def store_kernel(gate, up, norm, out_g, out_u, out_n, sem):
    copies = []
    rows = gate.shape[0] // 4
    for k in range(4):
        part = pl.ds(k * rows, rows)
        copies.append(pltpu.make_async_copy(gate.at[part], out_g.at[part], sem.at[2 * k]))
        copies.append(pltpu.make_async_copy(up.at[part], out_u.at[part], sem.at[2 * k + 1]))
    copies.append(pltpu.make_async_copy(norm, out_n, sem.at[8]))
    for copy in copies:
        copy.start()
    for copy in copies:
        copy.wait()


def body(train_gate, low_gate, high_gate, train_up, low_up, high_up, norm_train, norm_step):
    nz, nt = lax.axis_size("zero"), lax.axis_size("tp")
    depth, width = train_gate.shape
    rank = low_gate.shape[1]
    share = norm_train.shape[0]
    whole = nz * depth
    lines = depth // 128
    hbm = pl.BlockSpec(memory_space=pltpu.HBM)
    vmem = pl.BlockSpec(memory_space=pltpu.VMEM)
    dma = pltpu.SemaphoreType.DMA
    inputs = (
        train_gate, low_gate.T, high_gate, train_up, low_up.T, high_up,
        norm_train.reshape(1, share), norm_step.reshape(1, share),
    )
    gate, up, norm = pl.pallas_call(
        functools.partial(ring_kernel, nz, nt),
        out_shape=(
            pltpu.VMEM((width, whole), BF16),
            pltpu.VMEM((width, whole), BF16),
            pltpu.VMEM((nz * lines, 128), BF16),
        ),
        in_specs=[hbm] * 8,
        out_specs=(vmem,) * 3,
        scratch_shapes=[
            pltpu.VMEM((depth, width), BF16),
            pltpu.VMEM((depth, width), BF16),
            pltpu.VMEM((rank, depth), BF16),
            pltpu.VMEM((rank, depth), BF16),
            pltpu.VMEM((rank, width), BF16),
            pltpu.VMEM((rank, width), BF16),
            pltpu.VMEM((1, share), F32),
            pltpu.VMEM((1, share), F32),
            pltpu.VMEM((lines, 128), F32),
            pltpu.VMEM((nz, lines, 128), F32),
            pltpu.VMEM((nt, nz, lines, 128), F32),
            dma((7,)),
            dma((2,)),
            dma((2, SLOTS)),
            dma(()),
            dma(()),
            dma(()),
            pltpu.SemaphoreType.REGULAR((2,)),
        ],
        compiler_params=pltpu.CompilerParams(
            collective_id=0, has_side_effects=True, vmem_limit_bytes=24 * 1024 * 1024
        ),
    )(*(pltpu.with_memory_space_constraint(x, pltpu.HBM) for x in inputs))
    gate, up, norm = pl.pallas_call(
        store_kernel,
        out_shape=(
            jax.ShapeDtypeStruct((width, whole), BF16),
            jax.ShapeDtypeStruct((width, whole), BF16),
            jax.ShapeDtypeStruct((nz * lines, 128), BF16),
        ),
        in_specs=[vmem] * 3,
        out_specs=(hbm,) * 3,
        scratch_shapes=[dma((9,))],
        compiler_params=pltpu.CompilerParams(vmem_limit_bytes=24 * 1024 * 1024),
    )(gate, up, norm)
    return gate, up, norm.reshape(whole)


def solution(mesh):
    in_specs = (
        P(("shift", "zero"), "tp"),
        P(("shift", "zero"), None),
        P("shift", "tp"),
        P(("shift", "zero"), "tp"),
        P(("shift", "zero"), None),
        P("shift", "tp"),
        P(("shift", "zero", "tp")),
        P(("shift", "zero", "tp")),
    )
    out_specs = (P(("shift", "tp"), None), P(("shift", "tp"), None), P("shift"))
    return jax.shard_map(body, mesh=mesh, in_specs=in_specs, out_specs=out_specs, check_vma=False)
```

```python
import functools

import jax
import jax.numpy as jnp
from jax import lax
from jax.experimental import pallas as pl
from jax.experimental.pallas import tpu as pltpu
from jax.sharding import PartitionSpec as P

mix_rate = 0.5
MESH = pl.DeviceIdType.MESH
F32 = jnp.float32
BF16 = jnp.bfloat16
GATE, UP = 0, 1
RIGHT, LEFT = 0, 1

OWN = ((GATE, 0, 2), (GATE, 2, 8), (GATE, 8, 16), (UP, 0, 8), (UP, 8, 16))
OWN_GATE = 3
G0, G1, U0, U1 = (GATE, 0, 8), (GATE, 8, 16), (UP, 0, 8), (UP, 8, 16)
PASSED = (None, ((G0, G1, U0, U1), (G0, U0, G1, U1)), ((G0, G1, U0, U1), (U0, G0, U1, G1)))
SWAP_GATE, SWAP_UP = (GATE, 11, 16), (UP, 0, 3)
SLOTS = len(OWN) + 2 * 4 + 1


def ring_kernel(
    nz, nt,
    train_g, low_g, high_g, train_u, low_u, high_u, norm_a, norm_b,
    out_g, out_u, out_n,
    tg, tu, lg, lu, hg, hu, na, nb, n_own, n_hub, n_tp,
    in_sem, send_sem, recv_sem, sent_sem, came_sem, tp_sem, go,
):
    z = lax.axis_index("zero")
    t = lax.axis_index("tp")
    right, left = lax.rem(z + 1, nz), lax.rem(z + nz - 1, nz)
    toward = (right, left)
    depth, width = tg.shape
    part = width // 16
    hops = nz // 2
    end, sink = nz - 1, nz - 2

    outs = (out_g, out_u)
    sources = ((train_g, low_g, high_g), (train_u, low_u, high_u))
    holds = ((tg, lg, hg), (tu, lu, hu))

    head, tail = pl.ds(0, 2 * part), pl.ds(2 * part, 14 * part)
    first_high = pltpu.make_async_copy(high_g.at[:, head], hg.at[:, head], in_sem.at[1])
    loads = {
        (GATE, 1): pltpu.make_async_copy(low_g, lg, in_sem.at[0]),
        (GATE, 2): pltpu.make_async_copy(high_g.at[:, tail], hg.at[:, tail], in_sem.at[6]),
        (UP, 1): pltpu.make_async_copy(low_u, lu, in_sem.at[0]),
        (UP, 2): pltpu.make_async_copy(high_u, hu, in_sem.at[1]),
    }
    trains = []
    for p, a, b, k in ((GATE, 0, 2, 2), (GATE, 2, 16, 3), (UP, 0, 16, 2)):
        cols = pl.ds(a * part, (b - a) * part)
        trains.append(
            pltpu.make_async_copy(sources[p][0].at[:, cols], holds[p][0].at[:, cols], in_sem.at[k])
        )
    norm_loads = (
        pltpu.make_async_copy(norm_a, na, in_sem.at[4]),
        pltpu.make_async_copy(norm_b, nb, in_sem.at[5]),
    )
    trains[0].start()
    loads[GATE, 1].start()
    first_high.start()

    barrier = pltpu.get_barrier_semaphore()

    @pl.when(z == 0)
    def _():
        for k in range(1, nz):
            pl.semaphore_signal(barrier, inc=1, device_id={"zero": k}, device_id_type=MESH)
        for d in range(1, nt):
            pl.semaphore_signal(
                barrier, inc=1, device_id={"tp": lax.rem(t + d, nt)}, device_id_type=MESH
            )

    @pl.when((z > 0) & (z < sink))
    def _():
        pl.semaphore_signal(barrier, inc=1, device_id={"zero": right}, device_id_type=MESH)

    @pl.when(z == end)
    def _():
        pl.semaphore_signal(barrier, inc=1, device_id={"zero": left}, device_id_type=MESH)

    @pl.when(z > 0)
    def _():
        pl.semaphore_wait(
            barrier,
            1 + jnp.where((z > 1) & (z < end), 1, 0) + jnp.where(z == sink, 1, 0),
        )

    @pl.when((z > 0) & (z < end))
    def _():
        pl.semaphore_signal(go.at[LEFT], inc=1, device_id={"zero": left}, device_id_type=MESH)

    @pl.when(z >= sink)
    def _():
        pl.semaphore_signal(go.at[RIGHT], inc=1, device_id={"zero": right}, device_id_type=MESH)

    loads[GATE, 2].start()
    trains[1].start()
    for copy in norm_loads:
        copy.start()

    def where(origin, piece):
        p, a, b = piece
        first = pl.multiple_of(origin * depth, depth)
        return outs[p].at[pl.ds(a * part, (b - a) * part), pl.ds(first, depth)]

    def compute(piece):
        p, a, b = piece
        train, low, high = holds[p]
        cols = pl.ds(a * part, (b - a) * part)
        mixed = lax.dot_general(
            high[:, cols], low[...], (((0,), (0,)), ((), ())), preferred_element_type=F32
        )
        base = train[:, cols].T.astype(F32)
        where(z, piece)[...] = (base + mix_rate * mixed).astype(BF16)

    def slot(hop, i):
        return i if hop == 0 else SLOTS - 1 if hop == hops - 1 else len(OWN) + 4 * (hop - 1) + i

    def copy_of(way, hop, i, piece, back):
        gone = hop + back
        origin = lax.rem(z + nz - gone, nz) if way == RIGHT else lax.rem(z + gone, nz)
        block = where(origin, piece)
        return pltpu.make_async_remote_copy(
            src_ref=block, dst_ref=block,
            send_sem=send_sem.at[way],
            recv_sem=recv_sem.at[way, slot(hop, i)],
            device_id={"zero": toward[way]}, device_id_type=MESH,
        )

    right_first = (z == 0) | (z == end)

    def first_way(i):
        @pl.when(right_first)
        def _():
            copy_of(RIGHT, 0, i, OWN[i], 0).start()

        @pl.when(jnp.logical_not(right_first))
        def _():
            copy_of(LEFT, 0, i, OWN[i], 0).start()

    def second_way(i):
        @pl.when(right_first)
        def _():
            copy_of(LEFT, 0, i, OWN[i], 0).start()

        @pl.when(jnp.logical_not(right_first))
        def _():
            copy_of(RIGHT, 0, i, OWN[i], 0).start()

    loads[GATE, 1].wait()
    first_high.wait()
    trains[0].wait()
    compute(OWN[0])

    @pl.when(z == 0)
    def _():
        pl.semaphore_wait(go.at[LEFT], 1)

    first_way(0)
    loads[UP, 1].start()
    loads[UP, 2].start()
    trains[2].start()
    loads[GATE, 2].wait()
    trains[1].wait()
    compute(OWN[1])
    first_way(1)

    for copy in norm_loads:
        copy.wait()
    both = na[...] + nb[...]
    share = both.shape[1]
    line = jnp.concatenate([both] * (128 // share), axis=1)
    shape = n_own.shape
    spot = (
        lax.broadcasted_iota(jnp.int32, shape, 0) * 128
        + lax.broadcasted_iota(jnp.int32, shape, 1)
    )
    mine = (spot >= t * share) & (spot < (t + 1) * share)
    n_own[...] = jnp.where(mine, jnp.broadcast_to(line, shape), 0.0)
    to_hub = pltpu.make_async_remote_copy(
        src_ref=n_own, dst_ref=n_hub.at[z], send_sem=sent_sem, recv_sem=came_sem,
        device_id={"zero": 0}, device_id_type=MESH,
    )

    pl.when(z > 0)(to_hub.start)
    for i in range(2, OWN_GATE):
        compute(OWN[i])
        first_way(i)

    @pl.when((z > 0) & (z < sink))
    def _():
        pl.semaphore_wait(go.at[LEFT], 1)

    @pl.when((z == 0) | (z == end))
    def _():
        pl.semaphore_wait(go.at[RIGHT], 1)

    for i in range(OWN_GATE):
        second_way(i)

    loads[UP, 1].wait()
    loads[UP, 2].wait()
    trains[2].wait()
    for i in range(OWN_GATE, len(OWN)):
        compute(OWN[i])
        first_way(i)
        second_way(i)

    def to_all(k):
        return pltpu.make_async_remote_copy(
            src_ref=out_n, dst_ref=out_n, send_sem=sent_sem, recv_sem=came_sem,
            device_id={"zero": k}, device_id_type=MESH,
        )

    @pl.when(z == 0)
    def _():
        n_hub[0] = n_own[...]
        pl.semaphore_wait(barrier, nt - 1)
        rest = n_hub.at[pl.ds(1, nz - 1)]
        pltpu.make_async_remote_copy(
            src_ref=rest, dst_ref=rest, send_sem=sent_sem, recv_sem=came_sem,
            device_id={"zero": end}, device_id_type=MESH,
        ).wait_recv()
        for d in range(1, nt):
            pltpu.make_async_remote_copy(
                src_ref=n_hub, dst_ref=n_tp.at[d], send_sem=sent_sem, recv_sem=tp_sem,
                device_id={"tp": lax.rem(t + d, nt)}, device_id_type=MESH,
            ).start()
        rest = n_tp.at[pl.ds(1, nt - 1)]
        pltpu.make_async_remote_copy(
            src_ref=rest, dst_ref=rest, send_sem=sent_sem, recv_sem=tp_sem,
            device_id={"tp": lax.rem(t + 1, nt)}, device_id_type=MESH,
        ).wait()
        acc = n_hub[...]
        for d in range(1, nt):
            acc = acc + n_tp[d]
        out_n[...] = jnp.concatenate([acc[k] for k in range(nz)], axis=0).astype(BF16)
        for k in range(1, nz):
            to_all(k).start()

    def pieces_of(way, hop):
        return OWN if hop == 0 else PASSED[hop][way]

    def last_of(way, dest):
        if way == RIGHT:
            return (
                ((GATE, 0, SWAP_GATE[1]), None),
                (SWAP_GATE, dest != 0),
                (SWAP_UP, dest == end),
            )
        return (
            (SWAP_UP, dest != end),
            ((UP, SWAP_UP[2], 16), None),
            (SWAP_GATE, dest == 0),
        )

    def guarded(cond, act):
        if cond is None:
            act()
        else:
            pl.when(cond)(act)

    waited = set()

    def land(way, hop, piece):
        p, a, b = piece
        for i, (q, c, d) in enumerate(pieces_of(way, hop)):
            if q == p and c < b and d > a and (way, hop, i) not in waited:
                waited.add((way, hop, i))
                copy_of(way, hop, i, pieces_of(way, hop)[i], 1).wait_recv()

    for hop in range(1, hops - 1):
        for i in range(4):
            for way in (RIGHT, LEFT):
                piece = PASSED[hop][way][i]
                land(way, hop - 1, piece)
                copy_of(way, hop, i, piece, 0).start()

    hop = hops - 1
    for i in range(3):
        for way in (RIGHT, LEFT):
            piece, cond = last_of(way, toward[way])[i]
            land(way, hop - 1, piece)
            guarded(cond, copy_of(way, hop, i, piece, 0).start)
    for way in (RIGHT, LEFT):
        for p in (GATE, UP):
            land(way, hop - 1, (p, 0, 16))

    swap_gate, swap_up = (p[2] - p[1] for p in (SWAP_GATE, SWAP_UP))

    def total(way, dest, before, act):
        rows = part * depth // out_g.shape[1]
        base = before + 16 * rows
        more, less = (swap_up, swap_gate) if way == RIGHT else (swap_gate, swap_up)
        gains, loses = (end, 0) if way == RIGHT else (0, end)
        for cond, count in (
            (dest == gains, base + more * rows),
            (dest == loses, base - less * rows),
            ((dest != gains) & (dest != loses), base),
        ):
            block = out_g.at[pl.ds(0, count)]
            copy = pltpu.make_async_remote_copy(
                src_ref=block, dst_ref=block,
                send_sem=send_sem.at[way], recv_sem=recv_sem.at[way, SLOTS - 1],
                device_id={"zero": toward[way]}, device_id_type=MESH,
            )
            pl.when(cond)(functools.partial(act, copy))

    for way in (LEFT, RIGHT):
        total(way, z, 0, lambda copy: copy.wait_recv())
    for way in (RIGHT, LEFT):
        total(way, toward[way], (hops - 1) * 2 * depth * width // out_g.shape[1], lambda copy: copy.wait_send())

    @pl.when(z == 0)
    def _():
        sent = out_g.at[pl.ds(0, (nz - 1) * out_n.shape[0]), pl.ds(0, out_n.shape[1])]
        pltpu.make_async_remote_copy(
            src_ref=sent, dst_ref=sent, send_sem=sent_sem, recv_sem=came_sem,
            device_id={"zero": end}, device_id_type=MESH,
        ).wait_send()

    @pl.when(z > 0)
    def _():
        to_hub.wait_send()
        to_all(0).wait_recv()


def store_kernel(gate, up, norm, out_g, out_u, out_n, sem):
    copies = (
        pltpu.make_async_copy(gate, out_g, sem.at[0]),
        pltpu.make_async_copy(up, out_u, sem.at[1]),
        pltpu.make_async_copy(norm, out_n, sem.at[2]),
    )
    for copy in copies:
        copy.start()
    for copy in copies:
        copy.wait()


def body(train_gate, low_gate, high_gate, train_up, low_up, high_up, norm_train, norm_step):
    nz, nt = lax.axis_size("zero"), lax.axis_size("tp")
    depth, width = train_gate.shape
    rank = low_gate.shape[1]
    share = norm_train.shape[0]
    whole = nz * depth
    lines = depth // 128
    hbm = pl.BlockSpec(memory_space=pltpu.HBM)
    vmem = pl.BlockSpec(memory_space=pltpu.VMEM)
    dma = pltpu.SemaphoreType.DMA
    inputs = (
        train_gate, low_gate.T, high_gate, train_up, low_up.T, high_up,
        norm_train.reshape(1, share), norm_step.reshape(1, share),
    )
    gate, up, norm = pl.pallas_call(
        functools.partial(ring_kernel, nz, nt),
        out_shape=(
            pltpu.VMEM((width, whole), BF16),
            pltpu.VMEM((width, whole), BF16),
            pltpu.VMEM((nz * lines, 128), BF16),
        ),
        in_specs=[hbm] * 8,
        out_specs=(vmem,) * 3,
        scratch_shapes=[
            pltpu.VMEM((depth, width), BF16),
            pltpu.VMEM((depth, width), BF16),
            pltpu.VMEM((rank, depth), BF16),
            pltpu.VMEM((rank, depth), BF16),
            pltpu.VMEM((rank, width), BF16),
            pltpu.VMEM((rank, width), BF16),
            pltpu.VMEM((1, share), F32),
            pltpu.VMEM((1, share), F32),
            pltpu.VMEM((lines, 128), F32),
            pltpu.VMEM((nz, lines, 128), F32),
            pltpu.VMEM((nt, nz, lines, 128), F32),
            dma((7,)),
            dma((2,)),
            dma((2, SLOTS)),
            dma(()),
            dma(()),
            dma(()),
            pltpu.SemaphoreType.REGULAR((2,)),
        ],
        compiler_params=pltpu.CompilerParams(
            collective_id=0, has_side_effects=True, vmem_limit_bytes=24 * 1024 * 1024
        ),
    )(*(pltpu.with_memory_space_constraint(x, pltpu.HBM) for x in inputs))
    gate, up, norm = pl.pallas_call(
        store_kernel,
        out_shape=(
            jax.ShapeDtypeStruct((width, whole), BF16),
            jax.ShapeDtypeStruct((width, whole), BF16),
            jax.ShapeDtypeStruct((nz * lines, 128), BF16),
        ),
        in_specs=[vmem] * 3,
        out_specs=(hbm,) * 3,
        scratch_shapes=[dma((3,))],
        compiler_params=pltpu.CompilerParams(vmem_limit_bytes=24 * 1024 * 1024),
    )(gate, up, norm)
    return gate, up, norm.reshape(whole)


def solution(mesh):
    in_specs = (
        P(("shift", "zero"), "tp"),
        P(("shift", "zero"), None),
        P("shift", "tp"),
        P(("shift", "zero"), "tp"),
        P(("shift", "zero"), None),
        P("shift", "tp"),
        P(("shift", "zero", "tp")),
        P(("shift", "zero", "tp")),
    )
    out_specs = (P(("shift", "tp"), None), P(("shift", "tp"), None), P("shift"))
    return jax.shard_map(body, mesh=mesh, in_specs=in_specs, out_specs=out_specs, check_vma=False)
```

```python
import functools

import jax
import jax.numpy as jnp
from jax import lax
from jax.experimental import pallas as pl
from jax.experimental.pallas import tpu as pltpu
from jax.sharding import PartitionSpec as P

mix_rate = 0.5
MESH = pl.DeviceIdType.MESH
F32 = jnp.float32
BF16 = jnp.bfloat16
GATE, UP = 0, 1
RIGHT, LEFT = 0, 1

OWN = ((GATE, 0, 2), (GATE, 2, 8), (GATE, 8, 16), (UP, 0, 8), (UP, 8, 16))
OWN_GATE = 3
G0, G1, U0, U1 = (GATE, 0, 8), (GATE, 8, 16), (UP, 0, 8), (UP, 8, 16)
PASSED = (None, ((G0, G1, U0, U1), (G0, U0, G1, U1)), ((G0, G1, U0, U1), (U0, G0, U1, G1)))
SWAP_GATE, SWAP_UP = (GATE, 11, 16), (UP, 0, 3)
SLOTS = len(OWN) + 4 + 1
AGAIN, LAST_SLOT = ((SLOTS - 1, 0, 1, 2), (SLOTS - 1, 0, 1, 3)), (3, 2)


def ring_kernel(
    nz, nt,
    train_g, low_g, high_g, train_u, low_u, high_u, norm_a, norm_b,
    out_g, out_u, out_n,
    tg, tu, lg, lu, hg, hu, na, nb, n_own, n_hub, n_tp,
    in_sem, send_sem, recv_sem, sent_sem, came_sem, tp_sem, go,
):
    z = lax.axis_index("zero")
    t = lax.axis_index("tp")
    right, left = lax.rem(z + 1, nz), lax.rem(z + nz - 1, nz)
    toward = (right, left)
    depth, width = tg.shape
    part = width // 16
    hops = nz // 2
    end, sink = nz - 1, nz - 2

    outs = (out_g, out_u)
    sources = ((train_g, low_g, high_g), (train_u, low_u, high_u))
    holds = ((tg, lg, hg), (tu, lu, hu))

    head, tail = pl.ds(0, 2 * part), pl.ds(2 * part, 14 * part)
    first_high = pltpu.make_async_copy(high_g.at[:, head], hg.at[:, head], in_sem.at[1])
    loads = {
        (GATE, 1): pltpu.make_async_copy(low_g, lg, in_sem.at[0]),
        (GATE, 2): pltpu.make_async_copy(high_g.at[:, tail], hg.at[:, tail], in_sem.at[6]),
        (UP, 1): pltpu.make_async_copy(low_u, lu, in_sem.at[0]),
        (UP, 2): pltpu.make_async_copy(high_u, hu, in_sem.at[1]),
    }
    trains = []
    for p, a, b, k in ((GATE, 0, 2, 2), (GATE, 2, 16, 3), (UP, 0, 16, 2)):
        cols = pl.ds(a * part, (b - a) * part)
        trains.append(
            pltpu.make_async_copy(sources[p][0].at[:, cols], holds[p][0].at[:, cols], in_sem.at[k])
        )
    norm_loads = (
        pltpu.make_async_copy(norm_a, na, in_sem.at[4]),
        pltpu.make_async_copy(norm_b, nb, in_sem.at[5]),
    )
    trains[0].start()
    loads[GATE, 1].start()
    first_high.start()

    barrier = pltpu.get_barrier_semaphore()

    @pl.when(z == 0)
    def _():
        for k in range(1, nz):
            pl.semaphore_signal(barrier, inc=1, device_id={"zero": k}, device_id_type=MESH)
        for d in range(1, nt):
            pl.semaphore_signal(
                barrier, inc=1, device_id={"tp": lax.rem(t + d, nt)}, device_id_type=MESH
            )

    @pl.when((z > 0) & (z < sink))
    def _():
        pl.semaphore_signal(barrier, inc=1, device_id={"zero": right}, device_id_type=MESH)

    @pl.when(z == end)
    def _():
        pl.semaphore_signal(barrier, inc=1, device_id={"zero": left}, device_id_type=MESH)

    @pl.when(z > 0)
    def _():
        pl.semaphore_wait(
            barrier,
            1 + jnp.where((z > 1) & (z < end), 1, 0) + jnp.where(z == sink, 1, 0),
        )

    @pl.when((z > 0) & (z < end))
    def _():
        pl.semaphore_signal(go.at[LEFT], inc=1, device_id={"zero": left}, device_id_type=MESH)

    @pl.when(z >= sink)
    def _():
        pl.semaphore_signal(go.at[RIGHT], inc=1, device_id={"zero": right}, device_id_type=MESH)

    loads[GATE, 2].start()
    trains[1].start()
    for copy in norm_loads:
        copy.start()

    def where(origin, piece):
        p, a, b = piece
        first = pl.multiple_of(origin * depth, depth)
        return outs[p].at[pl.ds(a * part, (b - a) * part), pl.ds(first, depth)]

    def mix(piece):
        p, a, b = piece
        train, low, high = holds[p]
        return mix_rate * lax.dot_general(
            high[:, pl.ds(a * part, (b - a) * part)], low[...],
            (((0,), (0,)), ((), ())), preferred_element_type=F32,
        )

    def merge(piece, mixed):
        p, a, b = piece
        base = holds[p][0][:, pl.ds(a * part, (b - a) * part)].T.astype(F32)
        where(z, piece)[...] = (base + mixed).astype(BF16)

    def compute(piece):
        merge(piece, mix(piece))

    def slot(way, hop, i):
        if hop < 2:
            return len(OWN) * hop + i
        return AGAIN[way][i] if hop < hops - 1 else LAST_SLOT[way]

    def copy_of(way, hop, i, piece, back):
        gone = hop + back
        origin = lax.rem(z + nz - gone, nz) if way == RIGHT else lax.rem(z + gone, nz)
        block = where(origin, piece)
        return pltpu.make_async_remote_copy(
            src_ref=block, dst_ref=block,
            send_sem=send_sem.at[way],
            recv_sem=recv_sem.at[way, slot(way, hop, i)],
            device_id={"zero": toward[way]}, device_id_type=MESH,
        )

    right_first = (z == 0) | (z == end)

    def first_way(i):
        @pl.when(right_first)
        def _():
            copy_of(RIGHT, 0, i, OWN[i], 0).start()

        @pl.when(jnp.logical_not(right_first))
        def _():
            copy_of(LEFT, 0, i, OWN[i], 0).start()

    def second_way(i):
        @pl.when(right_first)
        def _():
            copy_of(LEFT, 0, i, OWN[i], 0).start()

        @pl.when(jnp.logical_not(right_first))
        def _():
            copy_of(RIGHT, 0, i, OWN[i], 0).start()

    loads[GATE, 1].wait()
    first_high.wait()
    mixed = mix(OWN[0])
    trains[0].wait()
    merge(OWN[0], mixed)

    @pl.when(z == 0)
    def _():
        pl.semaphore_wait(go.at[LEFT], 1)

    first_way(0)
    loads[UP, 1].start()
    loads[UP, 2].start()
    trains[2].start()
    loads[GATE, 2].wait()
    trains[1].wait()
    compute(OWN[1])
    first_way(1)

    for copy in norm_loads:
        copy.wait()
    both = na[...] + nb[...]
    share = both.shape[1]
    line = jnp.concatenate([both] * (128 // share), axis=1)
    shape = n_own.shape
    spot = (
        lax.broadcasted_iota(jnp.int32, shape, 0) * 128
        + lax.broadcasted_iota(jnp.int32, shape, 1)
    )
    mine = (spot >= t * share) & (spot < (t + 1) * share)
    n_own[...] = jnp.where(mine, jnp.broadcast_to(line, shape), 0.0)
    to_hub = pltpu.make_async_remote_copy(
        src_ref=n_own, dst_ref=n_hub.at[z], send_sem=sent_sem, recv_sem=came_sem,
        device_id={"zero": 0}, device_id_type=MESH,
    )

    pl.when(z > 0)(to_hub.start)
    for i in range(2, OWN_GATE):
        compute(OWN[i])
        first_way(i)

    @pl.when((z > 0) & (z < sink))
    def _():
        pl.semaphore_wait(go.at[LEFT], 1)

    @pl.when((z == 0) | (z == end))
    def _():
        pl.semaphore_wait(go.at[RIGHT], 1)

    for i in range(OWN_GATE):
        second_way(i)

    loads[UP, 1].wait()
    loads[UP, 2].wait()
    trains[2].wait()
    for i in range(OWN_GATE, len(OWN)):
        compute(OWN[i])
        first_way(i)
        second_way(i)

    def to_all(k):
        return pltpu.make_async_remote_copy(
            src_ref=out_n, dst_ref=out_n, send_sem=sent_sem, recv_sem=came_sem,
            device_id={"zero": k}, device_id_type=MESH,
        )

    @pl.when(z == 0)
    def _():
        n_hub[0] = n_own[...]
        pl.semaphore_wait(barrier, nt - 1)
        rest = n_hub.at[pl.ds(1, nz - 1)]
        pltpu.make_async_remote_copy(
            src_ref=rest, dst_ref=rest, send_sem=sent_sem, recv_sem=came_sem,
            device_id={"zero": end}, device_id_type=MESH,
        ).wait_recv()
        for d in range(1, nt):
            pltpu.make_async_remote_copy(
                src_ref=n_hub, dst_ref=n_tp.at[d], send_sem=sent_sem, recv_sem=tp_sem,
                device_id={"tp": lax.rem(t + d, nt)}, device_id_type=MESH,
            ).start()
        rest = n_tp.at[pl.ds(1, nt - 1)]
        pltpu.make_async_remote_copy(
            src_ref=rest, dst_ref=rest, send_sem=sent_sem, recv_sem=tp_sem,
            device_id={"tp": lax.rem(t + 1, nt)}, device_id_type=MESH,
        ).wait()
        acc = n_hub[...]
        for d in range(1, nt):
            acc = acc + n_tp[d]
        out_n[...] = jnp.concatenate([acc[k] for k in range(nz)], axis=0).astype(BF16)
        for k in range(1, nz):
            to_all(k).start()

    def pieces_of(way, hop):
        return OWN if hop == 0 else PASSED[hop][way]

    def last_of(way, dest):
        if way == RIGHT:
            return (
                ((GATE, 0, SWAP_GATE[1]), None),
                (SWAP_GATE, dest != 0),
                (SWAP_UP, dest == end),
            )
        return (
            (SWAP_UP, dest != end),
            ((UP, SWAP_UP[2], 16), None),
            (SWAP_GATE, dest == 0),
        )

    def guarded(cond, act):
        if cond is None:
            act()
        else:
            pl.when(cond)(act)

    waited = set()

    def land(way, hop, piece):
        p, a, b = piece
        for i, (q, c, d) in enumerate(pieces_of(way, hop)):
            if q == p and c < b and d > a and (way, hop, i) not in waited:
                waited.add((way, hop, i))
                copy_of(way, hop, i, pieces_of(way, hop)[i], 1).wait_recv()

    for hop in range(1, hops - 1):
        for i in range(4):
            for way in (RIGHT, LEFT):
                piece = PASSED[hop][way][i]
                land(way, hop - 1, piece)
                copy_of(way, hop, i, piece, 0).start()

    hop = hops - 1
    for i in range(3):
        for way in (RIGHT, LEFT):
            piece, cond = last_of(way, toward[way])[i]
            land(way, hop - 1, piece)
            guarded(cond, copy_of(way, hop, i, piece, 0).start)
    for way in (RIGHT, LEFT):
        for p in (GATE, UP):
            land(way, hop - 1, (p, 0, 16))

    swap_gate, swap_up = (p[2] - p[1] for p in (SWAP_GATE, SWAP_UP))

    def total(way, dest, before, act):
        rows = part * depth // out_g.shape[1]
        base = before + 16 * rows
        more, less = (swap_up, swap_gate) if way == RIGHT else (swap_gate, swap_up)
        gains, loses = (end, 0) if way == RIGHT else (0, end)
        for cond, count in (
            (dest == gains, base + more * rows),
            (dest == loses, base - less * rows),
            ((dest != gains) & (dest != loses), base),
        ):
            block = out_g.at[pl.ds(0, count)]
            copy = pltpu.make_async_remote_copy(
                src_ref=block, dst_ref=block,
                send_sem=send_sem.at[way], recv_sem=recv_sem.at[way, LAST_SLOT[way]],
                device_id={"zero": toward[way]}, device_id_type=MESH,
            )
            pl.when(cond)(functools.partial(act, copy))

    for way in (LEFT, RIGHT):
        total(way, z, 0, lambda copy: copy.wait_recv())
    for way in (RIGHT, LEFT):
        total(way, toward[way], (hops - 1) * 2 * depth * width // out_g.shape[1], lambda copy: copy.wait_send())

    @pl.when(z == 0)
    def _():
        sent = out_g.at[pl.ds(0, (nz - 1) * out_n.shape[0]), pl.ds(0, out_n.shape[1])]
        pltpu.make_async_remote_copy(
            src_ref=sent, dst_ref=sent, send_sem=sent_sem, recv_sem=came_sem,
            device_id={"zero": end}, device_id_type=MESH,
        ).wait_send()

    @pl.when(z > 0)
    def _():
        to_hub.wait_send()
        to_all(0).wait_recv()


def store_kernel(gate, up, norm, out_g, out_u, out_n, sem):
    copies = (
        pltpu.make_async_copy(gate, out_g, sem.at[0]),
        pltpu.make_async_copy(up, out_u, sem.at[1]),
        pltpu.make_async_copy(norm, out_n, sem.at[2]),
    )
    for copy in copies:
        copy.start()
    for copy in copies:
        copy.wait()


def body(train_gate, low_gate, high_gate, train_up, low_up, high_up, norm_train, norm_step):
    nz, nt = lax.axis_size("zero"), lax.axis_size("tp")
    depth, width = train_gate.shape
    rank = low_gate.shape[1]
    share = norm_train.shape[0]
    whole = nz * depth
    lines = depth // 128
    hbm = pl.BlockSpec(memory_space=pltpu.HBM)
    vmem = pl.BlockSpec(memory_space=pltpu.VMEM)
    dma = pltpu.SemaphoreType.DMA
    inputs = (
        train_gate, low_gate.T, high_gate, train_up, low_up.T, high_up,
        norm_train.reshape(1, share), norm_step.reshape(1, share),
    )
    gate, up, norm = pl.pallas_call(
        functools.partial(ring_kernel, nz, nt),
        out_shape=(
            pltpu.VMEM((width, whole), BF16),
            pltpu.VMEM((width, whole), BF16),
            pltpu.VMEM((nz * lines, 128), BF16),
        ),
        in_specs=[hbm] * 8,
        out_specs=(vmem,) * 3,
        scratch_shapes=[
            pltpu.VMEM((depth, width), BF16),
            pltpu.VMEM((depth, width), BF16),
            pltpu.VMEM((rank, depth), BF16),
            pltpu.VMEM((rank, depth), BF16),
            pltpu.VMEM((rank, width), BF16),
            pltpu.VMEM((rank, width), BF16),
            pltpu.VMEM((1, share), F32),
            pltpu.VMEM((1, share), F32),
            pltpu.VMEM((lines, 128), F32),
            pltpu.VMEM((nz, lines, 128), F32),
            pltpu.VMEM((nt, nz, lines, 128), F32),
            dma((7,)),
            dma((2,)),
            dma((2, SLOTS)),
            dma(()),
            dma(()),
            dma(()),
            pltpu.SemaphoreType.REGULAR((2,)),
        ],
        compiler_params=pltpu.CompilerParams(
            collective_id=0, has_side_effects=True, vmem_limit_bytes=24 * 1024 * 1024
        ),
    )(*(pltpu.with_memory_space_constraint(x, pltpu.HBM) for x in inputs))
    gate, up, norm = pl.pallas_call(
        store_kernel,
        out_shape=(
            jax.ShapeDtypeStruct((width, whole), BF16),
            jax.ShapeDtypeStruct((width, whole), BF16),
            jax.ShapeDtypeStruct((nz * lines, 128), BF16),
        ),
        in_specs=[vmem] * 3,
        out_specs=(hbm,) * 3,
        scratch_shapes=[dma((3,))],
        compiler_params=pltpu.CompilerParams(vmem_limit_bytes=24 * 1024 * 1024),
    )(gate, up, norm)
    return gate, up, norm.reshape(whole)


def solution(mesh):
    in_specs = (
        P(("shift", "zero"), "tp"),
        P(("shift", "zero"), None),
        P("shift", "tp"),
        P(("shift", "zero"), "tp"),
        P(("shift", "zero"), None),
        P("shift", "tp"),
        P(("shift", "zero", "tp")),
        P(("shift", "zero", "tp")),
    )
    out_specs = (P(("shift", "tp"), None), P(("shift", "tp"), None), P("shift"))
    return jax.shard_map(body, mesh=mesh, in_specs=in_specs, out_specs=out_specs, check_vma=False)
```
